32 devices in a mesh: dp: 8 (over z, x), section: 4 (over y, core).
Axes of the slice: x: 2, y: 2, z: 4, core: 2. Of those that a mesh axis runs over, the one named last changes fastest.
Arguments:
- entry_tokens: bfloat16 [8, 8, 16, 8192], P('dp'), may hold values from -6 to 6
- section_norm_gain: bfloat16 [4, 8192], P('section'), may hold values from 0.5 to 1.5
- adapter_down_weight: bfloat16 [4, 48, 8192], P('section'), may hold values from -0.0625 to 0.0625
- adapter_up_weight: bfloat16 [4, 48, 8192], P('section'), may hold values from -0.875 to 0.875
- output_gradient: bfloat16 [8, 8, 16, 8192], P('dp'), may hold values from -6 to 6
- lengths: int32 [8, 8], P('dp'), may hold values from 1 to 16
- keep: int32 [8, 4, 8, 16], P('dp', 'section'), may hold values from 0 to 1, as said below
Outputs:
- grad_up: float32 [4, 48, 8192], P('section')
- grad_gain: float32 [4, 8192], P('section')
The draws below stay inside these ranges and needn't reach their ends.
Inputs may be any that keep to these rules, and one draw needn't show every extreme that they name: `keep`: 0 or 1; token 0 of every microbatch is kept at every section.
All inputs are finite; a program needn't handle non-finite values.
Results may differ from the reference program's by a relative error of at most 0.02.
Values may be sent and summed in bfloat16 or wider, within the bound.
A program may use at most 64 MiB of HBM per device.

```python
import jax
import jax.numpy as jnp
from jax import lax

HIDDEN_WIDTH = 8192
ADAPTER_RANK = 48
TOK = 16
MICRO = 8
RELAY_SECTIONS = 4
GROUPS = 8


def draw_keep(key, part):
    ticket = jax.random.randint(key, (GROUPS, RELAY_SECTIONS, MICRO, TOK), 0, 5 * RELAY_SECTIONS)
    section_number = jnp.arange(RELAY_SECTIONS, dtype=jnp.int32)[None, :, None, None]
    limit = RELAY_SECTIONS + 3 * section_number
    position = jnp.arange(TOK, dtype=jnp.int32)[None, None, None, :]
    return jnp.where((ticket < limit) | (position == 0), 1, 0).astype(jnp.int32)


def touch_ends(array, key, least, high):
    spot = [jax.random.randint(jax.random.fold_in(key, axis), (), 0, length) for axis, length in enumerate(array.shape)]
    main_axis = array.shape.index(max(array.shape))
    neighbour = spot[:main_axis] + [(spot[main_axis] + 1) % array.shape[main_axis]] + spot[main_axis + 1:]
    return array.at[tuple(spot)].set(least).at[tuple(neighbour)].set(high)


def levels(key, extent, cuts, least, top_value):
    factor_of = 1.0
    for dim, shards_of in cuts:
        draws = jax.random.uniform(jax.random.fold_in(jax.random.fold_in(key, 6), dim), (shards_of,), jnp.float32, least / len(cuts), top_value / len(cuts))
        factor_of = factor_of * jnp.repeat(jnp.exp(draws), extent[dim] // shards_of).reshape((-1,) + (1,) * (len(extent) - 1 - dim))
    return factor_of


def noise(key, extent, spread, most, split=(), kind=jnp.bfloat16):
    values = jax.random.normal(key, extent, jnp.float32) * spread
    if len(split) > 0:
        values = levels(key, extent, split, -0.22, 0.18) * values
    return jnp.clip(values, min=-most, max=most).astype(kind)


def setup_inputs(seed: int = 0) -> dict:
    key_of = jax.random.split(jax.random.key(seed), 8)
    return {
        "entry_tokens": noise(key_of[0], (GROUPS, MICRO, TOK, HIDDEN_WIDTH), 1.0, 6.0, ((0, 8),)),
        "section_norm_gain": jnp.clip(1.0 + 0.1 * jax.random.normal(key_of[1], (RELAY_SECTIONS, HIDDEN_WIDTH), jnp.float32), 0.5, 1.5).astype(jnp.bfloat16),
        "adapter_down_weight": noise(key_of[2], (RELAY_SECTIONS, ADAPTER_RANK, HIDDEN_WIDTH), HIDDEN_WIDTH ** -0.5, 0.0625, ((0, 4),)),
        "adapter_up_weight": noise(key_of[3], (RELAY_SECTIONS, ADAPTER_RANK, HIDDEN_WIDTH), ADAPTER_RANK ** -0.5, 0.875, ((0, 4),)),
        "output_gradient": noise(key_of[4], (GROUPS, MICRO, TOK, HIDDEN_WIDTH), 1.0, 6.0, ((0, 8),)),
        "lengths": touch_ends(jax.random.randint(key_of[5], (GROUPS, MICRO), 1, TOK + 1), jax.random.fold_in(key_of[5], 1), 1, TOK).astype(jnp.int32),
        "keep": draw_keep(jax.random.fold_in(key_of[7], 71), 0),
    }


EPS = 1e-05

def forward_section(current_rows, gain_row, down_rows, up_rows, kept_rows):
    widened_rows = current_rows.astype(jnp.float32)
    inverse_norm = lax.rsqrt(lax.optimization_barrier(jnp.mean(widened_rows * widened_rows, axis=-1, keepdims=True)) + EPS)
    normed = (widened_rows * inverse_norm * gain_row.astype(jnp.float32)).astype(jnp.bfloat16)
    lowrank_rows = jnp.einsum('uwko,bo->uwkb', normed.astype(jnp.float32), down_rows.astype(jnp.float32)).astype(jnp.bfloat16)
    branch = jnp.einsum('jvau,ui->jvai', lowrank_rows.astype(jnp.float32), up_rows.astype(jnp.float32))
    weight = kept_rows[..., None]
    section_output = (widened_rows + weight * branch).astype(jnp.bfloat16)
    energy = lax.optimization_barrier(jnp.sum(weight * branch * branch, axis=(2, 3)))
    return (section_output, lowrank_rows, inverse_norm, widened_rows, energy)

def reference(entry_tokens, section_norm_gain, adapter_down_weight, adapter_up_weight, output_gradient, lengths, keep):
    position = jnp.arange(TOK, dtype=jnp.int32)
    valid_mask = (position[None, None, :] < lengths[:, :, None]).astype(jnp.float32)
    retained_mask = keep.astype(jnp.float32) * valid_mask[:, None]
    input_per_section = []
    energy = jnp.zeros((GROUPS, MICRO), jnp.float32)
    current_rows = entry_tokens
    for section_number in range(RELAY_SECTIONS):
        input_per_section.append(current_rows)
        current_rows, lowrank_rows, inverse_norm, widened_rows, section_power = forward_section(current_rows, section_norm_gain[section_number], adapter_down_weight[section_number], adapter_up_weight[section_number], retained_mask[:, section_number])
        energy = energy + section_power
    count = lax.optimization_barrier(jnp.sum(retained_mask, axis=(1, 3)))
    scaling = 1.0 / (count * jnp.sqrt(energy / (HIDDEN_WIDTH * count) + EPS))
    cotangent = (output_gradient.astype(jnp.float32) * valid_mask[..., None] * scaling[:, :, None, None]).astype(jnp.bfloat16)
    grads_up = []
    grads_gain = []
    for section_number in reversed(range(RELAY_SECTIONS)):
        section_output, lowrank_rows, inverse_norm, widened_rows, section_power = forward_section(input_per_section[section_number], section_norm_gain[section_number], adapter_down_weight[section_number], adapter_up_weight[section_number], retained_mask[:, section_number])
        weight = retained_mask[:, section_number][..., None]
        branch_gradient = (weight * cotangent.astype(jnp.float32)).astype(jnp.bfloat16)
        grad_section = jnp.einsum('gmtr,gmtd->rd', lowrank_rows.astype(jnp.float32), branch_gradient.astype(jnp.float32))
        lowrank_gradient = jnp.einsum('uwko,bo->uwkb', branch_gradient.astype(jnp.float32), adapter_up_weight[section_number].astype(jnp.float32)).astype(jnp.bfloat16)
        norm_gradient = jnp.einsum('jvau,ui->jvai', lowrank_gradient.astype(jnp.float32), adapter_down_weight[section_number].astype(jnp.float32))
        gain_grad = lax.optimization_barrier(jnp.sum(norm_gradient * widened_rows * inverse_norm, axis=(0, 1, 2)))
        scaled = norm_gradient * section_norm_gain[section_number].astype(jnp.float32)
        input_grad = inverse_norm * scaled - widened_rows * inverse_norm ** 3 * lax.optimization_barrier(jnp.mean(scaled * widened_rows, axis=-1, keepdims=True))
        cotangent = (cotangent.astype(jnp.float32) + input_grad).astype(jnp.bfloat16)
        grads_up.append(grad_section)
        grads_gain.append(gain_grad)
    grad_up = jnp.stack(grads_up[::-1])
    grad_gain = jnp.stack(grads_gain[::-1])
    return (grad_up, grad_gain)
```

```python
import functools

import jax
import jax.numpy as jnp
from jax import lax
from jax.experimental import pallas as pl
from jax.experimental.pallas import tpu as pltpu
from jax.sharding import PartitionSpec as P

EPS = 1e-05
NT = (((1,), (1,)), ((), ()))
TN = (((0,), (0,)), ((), ()))
MESH = pl.DeviceIdType.MESH
NN = (((1,), (0,)), ((), ()))


def mm(a, b, dims=NN, precision=None):
    return lax.dot_general(a, b, dims, precision=precision, preferred_element_type=jnp.float32)


def solve(au, uu, own, kept, valid, member, width, my):
    total, (rank, _) = len(au), au[0].shape
    rows = own[0].shape[1]
    bf = jnp.bfloat16
    norm2 = own[0][3 * rank:3 * rank + 1]
    r_now = jnp.concatenate([own[s][rank:2 * rank] for s in range(total)], axis=0)
    acc = jnp.concatenate([own[s][2 * rank:3 * rank] for s in range(total)], axis=0)
    zero = jnp.zeros((rank, rows), bf)
    cs, ps, invs, rs = [], [], [], []
    energy = jnp.zeros((1, rows), jnp.float32)
    count = jnp.zeros((1, rows), jnp.float32)
    for s in range(total):
        inv = lax.rsqrt(norm2 * (1.0 / width) + EPS)
        p = own[s][:rank]
        if s:
            p = p + mm(au[s], jnp.concatenate(cs + [zero] * (total - s), axis=0))
        c = (kept[s] * (p * inv).astype(bf).astype(jnp.float32)).astype(bf)
        cf = c.astype(jnp.float32)
        g = mm(uu[s], c, TN)
        quad = jnp.sum(cf * g[s * rank:(s + 1) * rank], axis=0, keepdims=True)
        cross = jnp.sum(cf * r_now[s * rank:(s + 1) * rank], axis=0, keepdims=True)
        rs.append(r_now)
        energy = energy + quad
        count = count + kept[s]
        norm2 = norm2 + 2.0 * cross + quad
        r_now = r_now + g
        cs.append(c)
        ps.append(p)
        invs.append(inv)
    sums = jnp.concatenate([energy, count, jnp.zeros((6, rows), jnp.float32)], axis=0)
    sums = mm(mm(sums, member, NT, lax.Precision.HIGHEST), member, NN, lax.Precision.HIGHEST)
    energy, count = sums[0:1], sums[1:2]
    scale = valid / (count * jnp.sqrt(energy / (width * count) + EPS))
    acc = acc * scale
    lams, alphas = [None] * total, [None] * total
    for s in reversed(range(total)):
        lam = (kept[s] * acc[s * rank:(s + 1) * rank]).astype(bf)
        lf = lam.astype(jnp.float32)
        alpha = invs[s] * invs[s] * invs[s] * jnp.sum(lf * ps[s], axis=0, keepdims=True) * (1.0 / width)
        lams[s] = (lf * invs[s]).astype(bf)
        alphas[s] = alpha
        if s:
            acc = acc + invs[s] * mm(au[s], lam, TN) - alpha * rs[s]
    c_all = jnp.concatenate(cs, axis=0)
    lam_all = jnp.concatenate(lams, axis=0)
    fl = lambda cond: jnp.where(cond, 1.0, 0.0).astype(jnp.float32)
    c_my = sum(fl(my == s) * cs[s].astype(jnp.float32) for s in range(total)).astype(bf)
    lam_my = sum(fl(my == s) * lams[s].astype(jnp.float32) for s in range(total)).astype(bf)
    beta = sum(fl(j > my) * alphas[j] for j in range(total))
    scaled_c = []
    for i in range(total):
        b = jnp.zeros((1, rows), jnp.float32)
        for j in range(i + 1, total):
            b = b + fl(j > my) * alphas[j]
        scaled_c.append((cs[i].astype(jnp.float32) * b).astype(bf))
    col = lax.broadcasted_iota(jnp.int32, (rank, total * rank), 1)
    mix = jnp.where(col < my * rank, mm(lam_my, c_all, NT),
                    jnp.where(col >= (my + 1) * rank, mm(c_my, lam_all, NT), 0.0))
    v = -mm(c_my, jnp.concatenate(scaled_c, axis=0), NT)
    m1 = (c_my.astype(jnp.float32) * scale).astype(bf)
    m2 = (-c_my.astype(jnp.float32) * beta).astype(bf)
    return m1, m2, lam_my, mix, v


def kernel(sizes, len_hbm, keep_hbm, gain_hbm, e_hbm, g_hbm, d_hbm, u_hbm, out_ref, gout_ref,
           len_ref, keep_ref, gain_ref, e_ref, g_ref, d_ref, u_ref, first_d, head, every, own_all, gram_tx, gram_rx, gram_all,
           tx, ttx, xrx, txrx, ztx, tztx, zrx, tzrx, mix_tx, mix_xrx, mix_ztx, mix_zrx, arx, tarx,
           load_sem, s1, r1, f1, s2, r2, s3, r3, s4, r4, sx, rx, stx, rtx, sz, rz, stz, rtz,
           smx, rmx, smz, rmz, sa, ra, sta, rta, sf, rf, stf, rtf):
    total, groups, inner, rank, micro, tok, width, part, model = sizes
    rows = micro * tok
    outer = groups // inner
    chunks = width // part
    tiles = part // 128
    bf, f32 = jnp.bfloat16, jnp.float32
    my = lax.axis_index("section")
    me = lax.axis_index("dp")
    z = me // inner
    x = me % inner

    def lanes(c):
        return pl.ds(pl.multiple_of(c * part, part), part)

    def ranks(s):
        return pl.ds(pl.multiple_of(s * rank, rank), rank)

    mine = jnp.minimum(me, chunks - 1)
    loads = [pltpu.make_async_copy(a, b, load_sem.at[i]) for i, (a, b) in enumerate(
        [(d_hbm.at[:, lanes(mine)], first_d), (u_hbm.at[:, lanes(mine)], head.at[1]),
         (e_hbm, e_ref), (d_hbm, d_ref), (u_hbm, u_ref), (g_hbm, g_ref),
         (gain_hbm, gain_ref), (keep_hbm, keep_ref), (len_hbm, len_ref)])]
    for load in loads:
        load.start()

    barrier = pltpu.get_barrier_semaphore()

    def greet_section(k, c):
        pl.semaphore_signal(barrier, inc=1, device_id={"section": (my + k) % total}, device_id_type=MESH)
        return c

    def greet_dp(k, c):
        pl.semaphore_signal(barrier, inc=1, device_id={"dp": (me + k) % groups}, device_id_type=MESH)
        return c

    lax.fori_loop(1, total, greet_section, 0)
    lax.fori_loop(1, groups, greet_dp, 0)

    def remote(src, dst, send, recv, **where):
        return pltpu.make_async_remote_copy(src_ref=src, dst_ref=dst, send_sem=send, recv_sem=recv,
                                            device_id=where, device_id_type=MESH)

    for i in (0, 1, 6, 7, 8):
        loads[i].wait()
    head[0] = (first_d[...].astype(f32) * gain_ref[:, lanes(mine)].astype(f32)).astype(bf)
    if chunks < groups:
        real = jnp.where(me < chunks, 1.0, 0.0).astype(f32)
        for i in range(2):
            head[i] = (head[i].astype(f32) * real).astype(bf)
    every[:, ranks(my), :] = head[...]

    lane = lax.broadcasted_iota(jnp.int32, (1, rows), 1)
    valid = jnp.zeros((1, rows), f32)
    for m in range(micro):
        valid = valid + jnp.where((lane >= m * tok) & (lane < m * tok + len_ref[0, m]), 1.0, 0.0)
    row8 = lax.broadcasted_iota(jnp.int32, (micro, rows), 0) * tok
    lane8 = lax.broadcasted_iota(jnp.int32, (micro, rows), 1)
    member = jnp.where((lane8 >= row8) & (lane8 < row8 + tok), 1.0, 0.0).astype(f32)
    row16 = lax.broadcasted_iota(jnp.int32, (tok, rows), 0)
    lane16 = lax.broadcasted_iota(jnp.int32, (tok, rows), 1)
    spread = jnp.zeros((tok, rows), f32)
    for m in range(micro):
        spread = spread + jnp.where(lane16 == row16 + m * tok, 1.0, 0.0)
    kept_row = valid * jnp.sum(mm(keep_ref[...].astype(f32), spread) * member, axis=0, keepdims=True)

    pl.semaphore_wait(barrier, total + groups - 2)

    step = 2 if total % 2 == 0 else 1
    mate = my + 1 - 2 * (my % 2)

    def weights(j, src):
        return remote(head, every.at[:, ranks(src), :], s1.at[j], r1.at[src], section=j)

    def share(src):
        return remote(every.at[:, ranks(src), :], every.at[:, ranks(src), :], f1.at[src], r1.at[src], section=mate)

    for k in range(step, total, step):
        weights((my + k) % total, my).start()
    if step == 2:
        weights(mate, my).start()

    loads[2].wait()
    loads[3].wait()
    loads[4].wait()

    def entry_chunk(c, acc):
        e = e_ref[:, lanes(c)]
        a = (d_ref[:, lanes(c)].astype(f32) * gain_ref[:, lanes(c)].astype(f32)).astype(bf)
        return (acc[0] + mm(jnp.concatenate([a, u_ref[:, lanes(c)]], axis=0), e, NT),
                acc[1] + mm(jnp.ones((8, part), bf), e * e, NT))

    zero = jnp.zeros((rank, rows), f32)
    sums = (jnp.zeros((2 * rank, rows), f32), jnp.zeros((8, rows), f32))
    sums = lax.fori_loop(0, chunks // 2, entry_chunk, sums)

    for k in range(step, total, step):
        src = (my + k) % total
        weights(my, src).wait_recv()
        if step == 2:
            share(src).start()

    def owns(j, src):
        return remote(own_all.at[src], own_all.at[src], s2.at[j], r2.at[src], section=j)

    if step == 2:
        for k in range(0, total, 2):
            weights(my, (mate + k) % total).wait_recv()
    gram_tx[...] = jnp.concatenate([mm(head[0], every[1], NT), mm(head[1], every[1], NT)], axis=0).astype(bf)

    def grams(j, src):
        return remote(gram_tx, gram_rx.at[src], s3.at[j], r3.at[src], dp=j)

    def send_gram(k, c):
        grams((me + k) % groups, me).start()
        return c

    lax.fori_loop(1, groups, send_gram, 0)

    aue, nn = lax.fori_loop(chunks // 2, chunks, entry_chunk, sums)
    loads[5].wait()
    ug = lax.fori_loop(0, chunks, lambda c, acc: acc + mm(u_ref[:, lanes(c)], g_ref[:, lanes(c)], NT), zero)
    own_all[my] = jnp.concatenate([aue, ug, nn, jnp.broadcast_to(kept_row, (8, rows))], axis=0)
    for k in range(1, total):
        owns((my + k) % total, my).start()

    gram_rx[me] = gram_tx[...]

    def wait_gram(k, c):
        grams(me, (me + k) % groups).wait_recv()
        return c

    lax.fori_loop(1, groups, wait_gram, 0)
    gram = lax.fori_loop(0, groups, lambda k, acc: acc + gram_rx[k].astype(f32),
                         jnp.zeros((2 * rank, total * rank), f32))
    gram_all[my] = gram.astype(bf)

    def all_grams(j, src):
        return remote(gram_all.at[src], gram_all.at[src], s4.at[j], r4.at[src], section=j)

    for k in range(1, total):
        all_grams((my + k) % total, my).start()
    for k in range(1, total):
        owns(my, (my + k) % total).wait_recv()
    for k in range(1, total):
        all_grams(my, (my + k) % total).wait_recv()

    au = [gram_all[s, :rank] for s in range(total)]
    uu = [gram_all[s, rank:] for s in range(total)]
    own = [own_all[s] for s in range(total)]
    kept = [own_all[s, 3 * rank + 8:3 * rank + 9] for s in range(total)]
    m1, m2, lam, mix, v = solve(au, uu, own, kept, valid, member, model, my)

    left = jnp.concatenate([jnp.concatenate([m1, m2], axis=1),
                            jnp.concatenate([jnp.zeros_like(lam), lam], axis=1)], axis=0)

    peer = me + 1 - 2 * x
    mix_tx[0] = mix.astype(bf)
    mix_tx[1] = v.astype(bf)

    def mix_x():
        return remote(mix_tx, mix_xrx, smx, rmx, dp=peer)

    def mix_z(j, src):
        return remote(mix_ztx, mix_zrx.at[src], smz.at[j], rmz.at[src], dp=j * inner + x)

    def piece(c):
        e = e_ref[:, lanes(c)]
        both = mm(left, jnp.concatenate([g_ref[:, lanes(c)], e], axis=0))
        row = jnp.sum(d_ref[:, lanes(c)].astype(f32) * both[rank:], axis=0, keepdims=True)
        return both[:rank], row

    def put_row(ref, row):
        for i in range(tiles):
            ref[i:i + 1, :] = row[:, 128 * i:128 * (i + 1)]

    def send_x(q):
        return (remote(tx.at[q], xrx.at[q], sx.at[q], rx.at[q], dp=peer),
                remote(ttx.at[q], txrx.at[q], stx.at[q], rtx.at[q], dp=peer))

    def send_z(q, src):
        return (remote(ztx.at[q], zrx.at[src], sz.at[q], rz.at[src], dp=q * inner + x),
                remote(tztx.at[q], tzrx.at[src], stz.at[q], rtz.at[src], dp=q * inner + x))

    if inner > 1:
        mix_x().start()

        def first(k, carry):
            q = (z + 1 + k) % outer
            c = q * inner + 1 - x
            big, row = piece(jnp.minimum(c, chunks - 1))
            tx[q] = big.astype(bf)
            put_row(ttx.at[q], row)
            for copy in send_x(q):
                copy.start()
            return carry

        lax.fori_loop(0, outer, first, 0)
        mix_x().wait_recv()
        for i in range(2):
            mix_ztx[i] = (mix_tx[i].astype(f32) + mix_xrx[i].astype(f32)).astype(bf)
    else:
        mix_ztx[...] = mix_tx[...]
    for k in range(1, outer):
        mix_z((z + k) % outer, z).start()

    def second(k, carry):
        q = (z + 1 + k) % outer
        big, row = piece(jnp.minimum(q * inner + x, chunks - 1))
        put_row(tztx.at[q], row)
        if inner > 1:
            for copy in send_x(q):
                copy.wait_recv()
            big = big + xrx[q].astype(f32)
            tztx[q, :tiles] = tztx[q, :tiles] + txrx[q, :tiles]
        ztx[q] = big.astype(bf)

        @pl.when(k < outer - 1)
        def _():
            for copy in send_z(q, z):
                copy.start()
        return carry

    lax.fori_loop(0, outer, second, 0)

    mixed = [mix_ztx[i].astype(f32) for i in range(2)]
    for k in range(1, outer):
        q = (z + k) % outer
        mix_z(z, q).wait_recv()
        mixed = [mixed[i] + mix_zrx[q, i].astype(f32) for i in range(2)]
    col = lax.broadcasted_iota(jnp.int32, (rank, total * rank), 1)
    low = jnp.where(col < my * rank, mixed[0], 0.0).astype(bf)
    high = jnp.where(col < my * rank, 0.0, mixed[0]).astype(bf)
    big = mm(high, every[0]) + mm(mixed[1].astype(bf), every[1]) + ztx[z].astype(f32)
    row = jnp.sum(d_ref[:, lanes(mine)].astype(f32) * mm(low, every[1]), axis=0, keepdims=True)
    put_row(tarx.at[me], row)
    tall = tarx[me, :tiles] + tztx[z, :tiles]
    for k in range(1, outer):
        q = (z + k) % outer
        for copy in send_z(z, q):
            copy.wait_recv()
        big = big + zrx[q].astype(f32)
        tall = tall + tzrx[q, :tiles]
    tarx[me, :tiles] = tall
    arx[me] = big.astype(bf)

    def gather_z(j, src):
        c = src * inner + x
        return (remote(arx.at[c], arx.at[c], sa.at[j], ra.at[src], dp=j * inner + x),
                remote(tarx.at[c], tarx.at[c], sta.at[j], rta.at[src], dp=j * inner + x))

    def gather_x(q, side):
        c = q * inner + side
        return (remote(arx.at[c], arx.at[c], sf.at[q], rf.at[q], dp=peer),
                remote(tarx.at[c], tarx.at[c], stf.at[q], rtf.at[q], dp=peer))

    def write(c):
        def go():
            out_ref[:, lanes(c)] = arx[c]
            for i in range(tiles):
                gout_ref[:, pl.ds(pl.multiple_of(c * part + 128 * i, 128), 128)] = tarx[c, i:i + 1, :]
        if chunks == groups:
            go()
        else:
            pl.when(c < chunks)(go)

    for k in range(1, outer):
        for copy in gather_z((z + k) % outer, z):
            copy.start()
    if inner > 1:
        for copy in gather_x(z, x):
            copy.start()
    write(me)

    def pass_on(k, carry):
        q = (z + k) % outer
        for copy in gather_z(z, q):
            copy.wait_recv()
        if inner > 1:
            for copy in gather_x(q, x):
                copy.start()
        write(q * inner + x)
        return carry

    lax.fori_loop(1, outer, pass_on, 0)

    if inner > 1:
        def last(k, carry):
            q = (z + k) % outer
            for copy in gather_x(q, 1 - x):
                copy.wait_recv()
            write(q * inner + 1 - x)
            return carry

        lax.fori_loop(0, outer, last, 0)

    for k in range(step, total, step):
        weights((my + k) % total, my).wait_send()
        if step == 2:
            share((my + k) % total).wait_send()
    if step == 2:
        weights(mate, my).wait_send()
    for k in range(1, total):
        j = (my + k) % total
        owns(j, my).wait_send()
        all_grams(j, my).wait_send()

    def left_dp(k, carry):
        grams((me + k) % groups, me).wait_send()
        return carry

    lax.fori_loop(1, groups, left_dp, 0)

    def left_z(k, carry):
        q = (z + k) % outer
        mix_z(q, z).wait_send()
        for copy in send_z(q, z) + gather_z(q, z):
            copy.wait_send()
        return carry

    lax.fori_loop(1, outer, left_z, 0)
    if inner > 1:
        mix_x().wait_send()

        def left_x(q, carry):
            for copy in send_x(q) + gather_x(q, x):
                copy.wait_send()
            return carry

        lax.fori_loop(0, outer, left_x, 0)


def body(entry, gain, down, up, gout, lengths, keep):
    bf, f32 = jnp.bfloat16, jnp.float32
    total = lax.axis_size("section")
    groups = lax.axis_size("dp")
    micro, tok, width = entry.shape[1:]
    rank = down.shape[1]
    rows = micro * tok
    part = 128 * (-(-width // (128 * groups)))
    pad = -width % part
    wide = width + pad
    inner = 2 if groups % 2 == 0 else 1
    outer = groups // inner
    widen = lambda a: jnp.pad(a, ((0, 0), (0, pad))) if pad else a
    hold = lambda a: pltpu.with_memory_space_constraint(a, pltpu.HBM)
    e = hold(widen(entry[0].reshape(rows, width)))
    go = hold(widen(gout[0].reshape(rows, width)))
    d, u = hold(widen(down[0])), hold(widen(up[0]))
    tall = max(8, part // 128)
    sizes = (total, groups, inner, rank, micro, tok, wide, part, width)
    vm = lambda *s, t=bf: pltpu.VMEM(s, t)
    dma = lambda *n: pltpu.SemaphoreType.DMA(n)
    scratch = [
        pltpu.SMEM((1, micro), jnp.int32), vm(micro, tok, t=jnp.int32), vm(1, wide),
        vm(rows, wide), vm(rows, wide), vm(rank, wide), vm(rank, wide),
        vm(rank, part), vm(2, rank, part), vm(2, total * rank, part),
        vm(total, 3 * rank + 16, rows, t=f32),
        vm(2 * rank, total * rank), vm(groups, 2 * rank, total * rank), vm(total, 2 * rank, total * rank),
        vm(outer, rank, part), vm(outer, tall, 128, t=f32), vm(outer, rank, part), vm(outer, tall, 128, t=f32),
        vm(outer, rank, part), vm(outer, tall, 128, t=f32), vm(outer, rank, part), vm(outer, tall, 128, t=f32),
        vm(2, rank, total * rank), vm(2, rank, total * rank), vm(2, rank, total * rank),
        vm(outer, 2, rank, total * rank),
        vm(groups, rank, part), vm(groups, tall, 128, t=f32),
        dma(9), dma(total), dma(total), dma(total), dma(total), dma(total), dma(groups), dma(groups), dma(total), dma(total),
        dma(outer), dma(outer), dma(outer), dma(outer), dma(outer), dma(outer), dma(outer), dma(outer),
        pltpu.SemaphoreType.DMA, pltpu.SemaphoreType.DMA, dma(outer), dma(outer),
        dma(outer), dma(outer), dma(outer), dma(outer), dma(outer), dma(outer), dma(outer), dma(outer),
    ]
    inside = pl.BlockSpec(memory_space=pltpu.VMEM)
    outside = pl.BlockSpec(memory_space=pltpu.HBM)
    up_grad, gain_grad = pl.pallas_call(
        functools.partial(kernel, sizes),
        out_shape=(jax.ShapeDtypeStruct((rank, wide), bf), jax.ShapeDtypeStruct((1, wide), f32)),
        in_specs=[outside] * 7,
        out_specs=(inside, inside),
        scratch_shapes=scratch,
        compiler_params=pltpu.CompilerParams(
            collective_id=0, has_side_effects=True, vmem_limit_bytes=48 * 1024 * 1024),
        name="relay",
    )(hold(lengths), hold(keep[0, 0]), hold(widen(gain)), e, go, d, u)
    return up_grad[None, :, :width].astype(f32), gain_grad[:, :width]


def solution(mesh):
    in_specs = (
        P("dp", None, None, None),
        P("section", None),
        P("section", None, None),
        P("section", None, None),
        P("dp", None, None, None),
        P("dp", None),
        P("dp", "section", None, None),
    )
    out_specs = (P("section", None, None), P("section", None))
    return jax.shard_map(body, mesh=mesh, in_specs=in_specs, out_specs=out_specs, check_vma=False)
```

```python
import functools

import jax
import jax.numpy as jnp
from jax import lax
from jax.experimental import pallas as pl
from jax.experimental.pallas import tpu as pltpu
from jax.sharding import PartitionSpec as P

EPS = 1e-05
NT = (((1,), (1,)), ((), ()))
TN = (((0,), (0,)), ((), ()))
MESH = pl.DeviceIdType.MESH
NN = (((1,), (0,)), ((), ()))


def mm(a, b, dims=NN, precision=None):
    return lax.dot_general(a, b, dims, precision=precision, preferred_element_type=jnp.float32)


def solve(au, uu, own, kept, valid, member, width, my):
    total, (rank, _) = len(au), au[0].shape
    rows = own[0].shape[1]
    bf = jnp.bfloat16
    norm2 = own[0][3 * rank:3 * rank + 1]
    r_now = jnp.concatenate([own[s][rank:2 * rank] for s in range(total)], axis=0)
    acc = jnp.concatenate([own[s][2 * rank:3 * rank] for s in range(total)], axis=0)
    zero = jnp.zeros((rank, rows), bf)
    cs, ps, invs, rs = [], [], [], []
    energy = jnp.zeros((1, rows), jnp.float32)
    count = jnp.zeros((1, rows), jnp.float32)
    for s in range(total):
        inv = lax.rsqrt(norm2 * (1.0 / width) + EPS)
        p = own[s][:rank]
        if s:
            p = p + mm(au[s], jnp.concatenate(cs + [zero] * (total - s), axis=0))
        c = (kept[s] * (p * inv).astype(bf).astype(jnp.float32)).astype(bf)
        cf = c.astype(jnp.float32)
        g = mm(uu[s], c, TN)
        quad = jnp.sum(cf * g[s * rank:(s + 1) * rank], axis=0, keepdims=True)
        cross = jnp.sum(cf * r_now[s * rank:(s + 1) * rank], axis=0, keepdims=True)
        rs.append(r_now)
        energy = energy + quad
        count = count + kept[s]
        norm2 = norm2 + 2.0 * cross + quad
        r_now = r_now + g
        cs.append(c)
        ps.append(p)
        invs.append(inv)
    sums = jnp.concatenate([energy, count, jnp.zeros((6, rows), jnp.float32)], axis=0)
    sums = mm(mm(sums, member, NT, lax.Precision.HIGHEST), member, NN, lax.Precision.HIGHEST)
    energy, count = sums[0:1], sums[1:2]
    scale = valid / (count * jnp.sqrt(energy / (width * count) + EPS))
    acc = acc * scale
    lams, alphas = [None] * total, [None] * total
    for s in reversed(range(total)):
        lam = (kept[s] * acc[s * rank:(s + 1) * rank]).astype(bf)
        lf = lam.astype(jnp.float32)
        alpha = invs[s] * invs[s] * invs[s] * jnp.sum(lf * ps[s], axis=0, keepdims=True) * (1.0 / width)
        lams[s] = (lf * invs[s]).astype(bf)
        alphas[s] = alpha
        if s:
            acc = acc + invs[s] * mm(au[s], lam, TN) - alpha * rs[s]
    c_all = jnp.concatenate(cs, axis=0)
    lam_all = jnp.concatenate(lams, axis=0)
    fl = lambda cond: jnp.where(cond, 1.0, 0.0).astype(jnp.float32)
    c_my = sum(fl(my == s) * cs[s].astype(jnp.float32) for s in range(total)).astype(bf)
    lam_my = sum(fl(my == s) * lams[s].astype(jnp.float32) for s in range(total)).astype(bf)
    beta = sum(fl(j > my) * alphas[j] for j in range(total))
    scaled_c = []
    for i in range(total):
        b = jnp.zeros((1, rows), jnp.float32)
        for j in range(i + 1, total):
            b = b + fl(j > my) * alphas[j]
        scaled_c.append((cs[i].astype(jnp.float32) * b).astype(bf))
    col = lax.broadcasted_iota(jnp.int32, (rank, total * rank), 1)
    mix = jnp.where(col < my * rank, mm(lam_my, c_all, NT),
                    jnp.where(col >= (my + 1) * rank, mm(c_my, lam_all, NT), 0.0))
    v = -mm(c_my, jnp.concatenate(scaled_c, axis=0), NT)
    m1 = (c_my.astype(jnp.float32) * scale).astype(bf)
    m2 = (-c_my.astype(jnp.float32) * beta).astype(bf)
    return m1, m2, lam_my, mix, v


def kernel(sizes, len_hbm, keep_hbm, gain_hbm, e_hbm, g_hbm, d_hbm, u_hbm, out_ref, gout_ref,
           len_ref, keep_ref, gain_ref, e_ref, g_ref, d_ref, u_ref, every, own_all, gram_tx, gram_rx, gram_all,
           tx, ttx, xrx, txrx, ztx, tztx, zrx, tzrx, mix_tx, mix_xrx, mix_ztx, mix_zrx, arx, tarx,
           load_sem, s1, r1, f1, s2, r2, s3, r3, s4, r4, sx, rx, stx, rtx, sz, rz, stz, rtz,
           smx, rmx, smz, rmz, sa, ra, sta, rta, sf, rf, stf, rtf):
    total, groups, inner, rank, micro, tok, width, part, model = sizes
    rows = micro * tok
    outer = groups // inner
    chunks = width // part
    tiles = part // 128
    bf, f32 = jnp.bfloat16, jnp.float32
    my = lax.axis_index("section")
    me = lax.axis_index("dp")
    z = me // inner
    x = me % inner

    def lanes(c):
        return pl.ds(pl.multiple_of(c * part, part), part)

    def ranks(s):
        return pl.ds(pl.multiple_of(s * rank, rank), rank)

    mine = jnp.minimum(me, chunks - 1)
    loads = [pltpu.make_async_copy(a, b, load_sem.at[i]) for i, (a, b) in enumerate(
        [(u_hbm.at[:, lanes(mine)], every.at[1, ranks(my), :]),
         (gain_hbm, gain_ref), (keep_hbm, keep_ref), (len_hbm, len_ref),
         (e_hbm, e_ref), (d_hbm, d_ref), (u_hbm, u_ref), (g_hbm, g_ref)])]
    for load in loads:
        load.start()

    barrier = pltpu.get_barrier_semaphore()

    def greet_section(k, c):
        pl.semaphore_signal(barrier, inc=1, device_id={"section": (my + k) % total}, device_id_type=MESH)
        return c

    def greet_dp(k, c):
        pl.semaphore_signal(barrier, inc=1, device_id={"dp": (me + k) % groups}, device_id_type=MESH)
        return c

    lax.fori_loop(1, total, greet_section, 0)
    lax.fori_loop(1, groups, greet_dp, 0)

    def remote(src, dst, send, recv, **where):
        return pltpu.make_async_remote_copy(src_ref=src, dst_ref=dst, send_sem=send, recv_sem=recv,
                                            device_id=where, device_id_type=MESH)

    for i in range(4):
        loads[i].wait()
    real = jnp.where(me < chunks, 1.0, 0.0).astype(f32)
    if chunks < groups:
        every[1, ranks(my), :] = (every[1, ranks(my), :].astype(f32) * real).astype(bf)

    lane = lax.broadcasted_iota(jnp.int32, (1, rows), 1)
    valid = jnp.zeros((1, rows), f32)
    for m in range(micro):
        valid = valid + jnp.where((lane >= m * tok) & (lane < m * tok + len_ref[0, m]), 1.0, 0.0)
    row8 = lax.broadcasted_iota(jnp.int32, (micro, rows), 0) * tok
    lane8 = lax.broadcasted_iota(jnp.int32, (micro, rows), 1)
    member = jnp.where((lane8 >= row8) & (lane8 < row8 + tok), 1.0, 0.0).astype(f32)
    row16 = lax.broadcasted_iota(jnp.int32, (tok, rows), 0)
    lane16 = lax.broadcasted_iota(jnp.int32, (tok, rows), 1)
    spread = jnp.zeros((tok, rows), f32)
    for m in range(micro):
        spread = spread + jnp.where(lane16 == row16 + m * tok, 1.0, 0.0)
    kept_row = valid * jnp.sum(mm(keep_ref[...].astype(f32), spread) * member, axis=0, keepdims=True)

    pl.semaphore_wait(barrier, total + groups - 2)

    step = 2 if total % 2 == 0 else 1
    mate = my + 1 - 2 * (my % 2)

    def block(w, src):
        return every.at[w, ranks(src), :]

    def weights(w, j, src):
        return remote(block(w, src), block(w, src), s1.at[w, j], r1.at[w, src], section=j)

    def share(w, src):
        return remote(block(w, src), block(w, src), f1.at[w, src], r1.at[w, src], section=mate)

    def send_weights(w):
        for k in range(step, total, step):
            weights(w, (my + k) % total, my).start()
        if step == 2:
            weights(w, mate, my).start()

    def pass_weights(w):
        for k in range(step, total, step):
            src = (my + k) % total
            weights(w, my, src).wait_recv()
            if step == 2:
                share(w, src).start()

    def wait_weights(w):
        if step == 2:
            for k in range(0, total, 2):
                weights(w, my, (mate + k) % total).wait_recv()

    send_weights(1)
    for i in range(4, 7):
        loads[i].wait()

    def entry_chunk(c, acc):
        e = e_ref[:, lanes(c)]
        a = (d_ref[:, lanes(c)].astype(f32) * gain_ref[:, lanes(c)].astype(f32)).astype(bf)
        return (acc[0] + mm(jnp.concatenate([a, u_ref[:, lanes(c)]], axis=0), e, NT),
                acc[1] + mm(jnp.ones((8, part), bf), e * e, NT))

    zero = jnp.zeros((rank, rows), f32)
    sums = (jnp.zeros((2 * rank, rows), f32), jnp.zeros((8, rows), f32))
    aue, nn = lax.fori_loop(0, chunks, entry_chunk, sums)
    loads[7].wait()
    ug = lax.fori_loop(0, chunks, lambda c, acc: acc + mm(u_ref[:, lanes(c)], g_ref[:, lanes(c)], NT), zero)
    own_all[my] = jnp.concatenate([aue, ug, nn, jnp.broadcast_to(kept_row, (8, rows))], axis=0)

    def owns(j, src):
        return remote(own_all.at[src], own_all.at[src], s2.at[j], r2.at[src], section=j)

    for k in range(1, total):
        owns((my + k) % total, my).start()
    every[0, ranks(my), :] = (d_ref[:, lanes(mine)].astype(f32) * gain_ref[:, lanes(mine)].astype(f32)
                              * real).astype(bf)
    send_weights(0)

    pass_weights(1)
    wait_weights(1)
    size = total * rank
    col = lax.broadcasted_iota(jnp.int32, (rank, size), 1)
    both = mm(jnp.concatenate([every[0, ranks(my), :], every[1, ranks(my), :]], axis=0), every[1], NT)
    gram_tx[...] = jnp.where(col < my * rank, both[:rank], both[rank:]).astype(bf)

    def grams(j, src):
        return remote(gram_tx, gram_rx.at[src], s3.at[j], r3.at[src], dp=j)

    def send_gram(k, c):
        grams((me + k) % groups, me).start()
        return c

    lax.fori_loop(1, groups, send_gram, 0)
    pass_weights(0)
    gram_rx[me] = gram_tx[...]

    def wait_gram(k, c):
        grams(me, (me + k) % groups).wait_recv()
        return c

    lax.fori_loop(1, groups, wait_gram, 0)
    gram = lax.fori_loop(0, groups, lambda k, acc: acc + gram_rx[k].astype(f32), jnp.zeros((rank, size), f32))
    gram_all[ranks(my), :] = gram.astype(bf)

    def all_grams(j, src):
        return remote(gram_all.at[ranks(src), :], gram_all.at[ranks(src), :], s4.at[j], r4.at[src], section=j)

    for k in range(1, total):
        all_grams((my + k) % total, my).start()
    for k in range(1, total):
        owns(my, (my + k) % total).wait_recv()
    for k in range(1, total):
        all_grams(my, (my + k) % total).wait_recv()

    table = gram_all[...]
    eye = jnp.where(lax.broadcasted_iota(jnp.int32, (size, size), 0)
                    == lax.broadcasted_iota(jnp.int32, (size, size), 1), 1.0, 0.0).astype(bf)
    turned = mm(table, eye, TN)
    au = [table[s * rank:(s + 1) * rank] for s in range(total)]
    uu = [jnp.where(col >= s * rank, au[s].astype(f32), turned[s * rank:(s + 1) * rank]).astype(bf)
          for s in range(total)]
    own = [own_all[s] for s in range(total)]
    kept = [own_all[s, 3 * rank + 8:3 * rank + 9] for s in range(total)]
    m1, m2, lam, mix, v = solve(au, uu, own, kept, valid, member, model, my)

    left = jnp.concatenate([jnp.concatenate([m1, m2], axis=1),
                            jnp.concatenate([jnp.zeros_like(lam), lam], axis=1)], axis=0)

    peer = me + 1 - 2 * x
    mix_tx[0] = mix.astype(bf)
    mix_tx[1] = v.astype(bf)

    def mix_x():
        return remote(mix_tx, mix_xrx, smx, rmx, dp=peer)

    def mix_z(j, src):
        return remote(mix_ztx, mix_zrx.at[src], smz.at[j], rmz.at[src], dp=j * inner + x)

    def piece(c):
        e = e_ref[:, lanes(c)]
        both = mm(left, jnp.concatenate([g_ref[:, lanes(c)], e], axis=0))
        row = jnp.sum(d_ref[:, lanes(c)].astype(f32) * both[rank:], axis=0, keepdims=True)
        return both[:rank], row

    def put_row(ref, row):
        for i in range(tiles):
            ref[i:i + 1, :] = row[:, 128 * i:128 * (i + 1)]

    def send_x(q):
        return (remote(tx.at[q], xrx.at[q], sx.at[q], rx.at[q], dp=peer),
                remote(ttx.at[q], txrx.at[q], stx.at[q], rtx.at[q], dp=peer))

    def send_z(q, src):
        return (remote(ztx.at[q], zrx.at[src], sz.at[q], rz.at[src], dp=q * inner + x),
                remote(tztx.at[q], tzrx.at[src], stz.at[q], rtz.at[src], dp=q * inner + x))

    if inner > 1:
        mix_x().start()

        def first(k, carry):
            q = (z + 1 + k) % outer
            c = q * inner + 1 - x
            big, row = piece(jnp.minimum(c, chunks - 1))
            tx[q] = big.astype(bf)
            put_row(ttx.at[q], row)
            for copy in send_x(q):
                copy.start()
            return carry

        lax.fori_loop(0, outer, first, 0)
        mix_x().wait_recv()
        for i in range(2):
            mix_ztx[i] = (mix_tx[i].astype(f32) + mix_xrx[i].astype(f32)).astype(bf)
    else:
        mix_ztx[...] = mix_tx[...]
    for k in range(1, outer):
        mix_z((z + k) % outer, z).start()

    def second(k, carry):
        q = (z + 1 + k) % outer
        big, row = piece(jnp.minimum(q * inner + x, chunks - 1))
        put_row(tztx.at[q], row)
        if inner > 1:
            for copy in send_x(q):
                copy.wait_recv()
            big = big + xrx[q].astype(f32)
            tztx[q, :tiles] = tztx[q, :tiles] + txrx[q, :tiles]
        ztx[q] = big.astype(bf)

        @pl.when(k < outer - 1)
        def _():
            for copy in send_z(q, z):
                copy.start()
        return carry

    lax.fori_loop(0, outer, second, 0)

    wait_weights(0)
    mixed = [mix_ztx[i].astype(f32) for i in range(2)]
    for k in range(1, outer):
        q = (z + k) % outer
        mix_z(z, q).wait_recv()
        mixed = [mixed[i] + mix_zrx[q, i].astype(f32) for i in range(2)]
    col = lax.broadcasted_iota(jnp.int32, (rank, total * rank), 1)
    low = jnp.where(col < my * rank, mixed[0], 0.0).astype(bf)
    high = jnp.where(col < my * rank, 0.0, mixed[0]).astype(bf)
    big = mm(high, every[0]) + mm(mixed[1].astype(bf), every[1]) + ztx[z].astype(f32)
    row = jnp.sum(d_ref[:, lanes(mine)].astype(f32) * mm(low, every[1]), axis=0, keepdims=True)
    put_row(tarx.at[me], row)
    tall = tarx[me, :tiles] + tztx[z, :tiles]
    for k in range(1, outer):
        q = (z + k) % outer
        for copy in send_z(z, q):
            copy.wait_recv()
        big = big + zrx[q].astype(f32)
        tall = tall + tzrx[q, :tiles]
    tarx[me, :tiles] = tall
    arx[me] = big.astype(bf)

    def gather_z(j, src):
        c = src * inner + x
        return (remote(arx.at[c], arx.at[c], sa.at[j], ra.at[src], dp=j * inner + x),
                remote(tarx.at[c], tarx.at[c], sta.at[j], rta.at[src], dp=j * inner + x))

    def gather_x(q, side):
        c = q * inner + side
        return (remote(arx.at[c], arx.at[c], sf.at[q], rf.at[q], dp=peer),
                remote(tarx.at[c], tarx.at[c], stf.at[q], rtf.at[q], dp=peer))

    def write(c):
        def go():
            out_ref[:, lanes(c)] = arx[c]
            for i in range(tiles):
                gout_ref[:, pl.ds(pl.multiple_of(c * part + 128 * i, 128), 128)] = tarx[c, i:i + 1, :]
        if chunks == groups:
            go()
        else:
            pl.when(c < chunks)(go)

    for k in range(1, outer):
        for copy in gather_z((z + k) % outer, z):
            copy.start()
    if inner > 1:
        for copy in gather_x(z, x):
            copy.start()
    write(me)

    def pass_on(k, carry):
        q = (z + k) % outer
        for copy in gather_z(z, q):
            copy.wait_recv()
        if inner > 1:
            for copy in gather_x(q, x):
                copy.start()
        write(q * inner + x)
        return carry

    lax.fori_loop(1, outer, pass_on, 0)

    if inner > 1:
        def last(k, carry):
            q = (z + k) % outer
            for copy in gather_x(q, 1 - x):
                copy.wait_recv()
            write(q * inner + 1 - x)
            return carry

        lax.fori_loop(0, outer, last, 0)

    for w in range(2):
        for k in range(step, total, step):
            weights(w, (my + k) % total, my).wait_send()
            if step == 2:
                share(w, (my + k) % total).wait_send()
        if step == 2:
            weights(w, mate, my).wait_send()
    for k in range(1, total):
        j = (my + k) % total
        owns(j, my).wait_send()
        all_grams(j, my).wait_send()

    def left_dp(k, carry):
        grams((me + k) % groups, me).wait_send()
        return carry

    lax.fori_loop(1, groups, left_dp, 0)

    def left_z(k, carry):
        q = (z + k) % outer
        mix_z(q, z).wait_send()
        for copy in send_z(q, z) + gather_z(q, z):
            copy.wait_send()
        return carry

    lax.fori_loop(1, outer, left_z, 0)
    if inner > 1:
        mix_x().wait_send()

        def left_x(q, carry):
            for copy in send_x(q) + gather_x(q, x):
                copy.wait_send()
            return carry

        lax.fori_loop(0, outer, left_x, 0)


def body(entry, gain, down, up, gout, lengths, keep):
    bf, f32 = jnp.bfloat16, jnp.float32
    total = lax.axis_size("section")
    groups = lax.axis_size("dp")
    micro, tok, width = entry.shape[1:]
    rank = down.shape[1]
    rows = micro * tok
    part = 128 * (-(-width // (128 * groups)))
    pad = -width % part
    wide = width + pad
    inner = 2 if groups % 2 == 0 else 1
    outer = groups // inner
    widen = lambda a: jnp.pad(a, ((0, 0), (0, pad))) if pad else a
    hold = lambda a: pltpu.with_memory_space_constraint(a, pltpu.HBM)
    e = hold(widen(entry[0].reshape(rows, width)))
    go = hold(widen(gout[0].reshape(rows, width)))
    d, u = hold(widen(down[0])), hold(widen(up[0]))
    tall = max(8, part // 128)
    sizes = (total, groups, inner, rank, micro, tok, wide, part, width)
    vm = lambda *s, t=bf: pltpu.VMEM(s, t)
    dma = lambda *n: pltpu.SemaphoreType.DMA(n)
    scratch = [
        pltpu.SMEM((1, micro), jnp.int32), vm(micro, tok, t=jnp.int32), vm(1, wide),
        vm(rows, wide), vm(rows, wide), vm(rank, wide), vm(rank, wide),
        vm(2, total * rank, part),
        vm(total, 3 * rank + 16, rows, t=f32),
        vm(rank, total * rank), vm(groups, rank, total * rank), vm(total * rank, total * rank),
        vm(outer, rank, part), vm(outer, tall, 128, t=f32), vm(outer, rank, part), vm(outer, tall, 128, t=f32),
        vm(outer, rank, part), vm(outer, tall, 128, t=f32), vm(outer, rank, part), vm(outer, tall, 128, t=f32),
        vm(2, rank, total * rank), vm(2, rank, total * rank), vm(2, rank, total * rank),
        vm(outer, 2, rank, total * rank),
        vm(groups, rank, part), vm(groups, tall, 128, t=f32),
        dma(8), dma(2, total), dma(2, total), dma(2, total), dma(total), dma(total), dma(groups), dma(groups), dma(total), dma(total),
        dma(outer), dma(outer), dma(outer), dma(outer), dma(outer), dma(outer), dma(outer), dma(outer),
        pltpu.SemaphoreType.DMA, pltpu.SemaphoreType.DMA, dma(outer), dma(outer),
        dma(outer), dma(outer), dma(outer), dma(outer), dma(outer), dma(outer), dma(outer), dma(outer),
    ]
    inside = pl.BlockSpec(memory_space=pltpu.VMEM)
    outside = pl.BlockSpec(memory_space=pltpu.HBM)
    up_grad, gain_grad = pl.pallas_call(
        functools.partial(kernel, sizes),
        out_shape=(jax.ShapeDtypeStruct((rank, wide), bf), jax.ShapeDtypeStruct((1, wide), f32)),
        in_specs=[outside] * 7,
        out_specs=(inside, inside),
        scratch_shapes=scratch,
        compiler_params=pltpu.CompilerParams(
            collective_id=0, has_side_effects=True, vmem_limit_bytes=48 * 1024 * 1024),
        name="relay",
    )(hold(lengths), hold(keep[0, 0]), hold(widen(gain)), e, go, d, u)
    return up_grad[None, :, :width].astype(f32), gain_grad[:, :width]


def solution(mesh):
    in_specs = (
        P("dp", None, None, None),
        P("section", None),
        P("section", None, None),
        P("section", None, None),
        P("dp", None, None, None),
        P("dp", None),
        P("dp", "section", None, None),
    )
    out_specs = (P("section", None, None), P("section", None))
    return jax.shard_map(body, mesh=mesh, in_specs=in_specs, out_specs=out_specs, check_vma=False)
```

```python
import functools

import jax
import jax.numpy as jnp
from jax import lax
from jax.experimental import pallas as pl
from jax.experimental.pallas import tpu as pltpu
from jax.sharding import PartitionSpec as P

EPS = 1e-05
NT = (((1,), (1,)), ((), ()))
TN = (((0,), (0,)), ((), ()))
MESH = pl.DeviceIdType.MESH
NN = (((1,), (0,)), ((), ()))


def mm(a, b, dims=NN, precision=None):
    return lax.dot_general(a, b, dims, precision=precision, preferred_element_type=jnp.float32)


def solve(au, uu, own, kept, valid, member, width, my):
    total, (rank, _) = len(au), au[0].shape
    rows = own[0].shape[1]
    bf = jnp.bfloat16
    norm2 = own[0][3 * rank:3 * rank + 1]
    r_now = jnp.concatenate([own[s][rank:2 * rank] for s in range(total)], axis=0)
    acc = jnp.concatenate([own[s][2 * rank:3 * rank] for s in range(total)], axis=0)
    zero = jnp.zeros((rank, rows), bf)
    cs, ps, invs, rs = [], [], [], []
    energy = jnp.zeros((1, rows), jnp.float32)
    count = jnp.zeros((1, rows), jnp.float32)
    for s in range(total):
        inv = lax.rsqrt(norm2 * (1.0 / width) + EPS)
        p = own[s][:rank]
        if s:
            p = p + mm(au[s], jnp.concatenate(cs + [zero] * (total - s), axis=0))
        c = (kept[s] * (p * inv).astype(bf).astype(jnp.float32)).astype(bf)
        cf = c.astype(jnp.float32)
        g = mm(uu[s], c, TN)
        quad = jnp.sum(cf * g[s * rank:(s + 1) * rank], axis=0, keepdims=True)
        cross = jnp.sum(cf * r_now[s * rank:(s + 1) * rank], axis=0, keepdims=True)
        rs.append(r_now)
        energy = energy + quad
        count = count + kept[s]
        norm2 = norm2 + 2.0 * cross + quad
        r_now = r_now + g
        cs.append(c)
        ps.append(p)
        invs.append(inv)
    sums = jnp.concatenate([energy, count, jnp.zeros((6, rows), jnp.float32)], axis=0)
    sums = mm(mm(sums, member, NT, lax.Precision.HIGHEST), member, NN, lax.Precision.HIGHEST)
    energy, count = sums[0:1], sums[1:2]
    scale = valid / (count * jnp.sqrt(energy / (width * count) + EPS))
    acc = acc * scale
    lams, alphas = [None] * total, [None] * total
    for s in reversed(range(total)):
        lam = (kept[s] * acc[s * rank:(s + 1) * rank]).astype(bf)
        lf = lam.astype(jnp.float32)
        alpha = invs[s] * invs[s] * invs[s] * jnp.sum(lf * ps[s], axis=0, keepdims=True) * (1.0 / width)
        lams[s] = (lf * invs[s]).astype(bf)
        alphas[s] = alpha
        if s:
            acc = acc + invs[s] * mm(au[s], lam, TN) - alpha * rs[s]
    c_all = jnp.concatenate(cs, axis=0)
    lam_all = jnp.concatenate(lams, axis=0)
    fl = lambda cond: jnp.where(cond, 1.0, 0.0).astype(jnp.float32)
    c_my = sum(fl(my == s) * cs[s].astype(jnp.float32) for s in range(total)).astype(bf)
    lam_my = sum(fl(my == s) * lams[s].astype(jnp.float32) for s in range(total)).astype(bf)
    beta = sum(fl(j > my) * alphas[j] for j in range(total))
    scaled_c = []
    for i in range(total):
        b = jnp.zeros((1, rows), jnp.float32)
        for j in range(i + 1, total):
            b = b + fl(j > my) * alphas[j]
        scaled_c.append((cs[i].astype(jnp.float32) * b).astype(bf))
    col = lax.broadcasted_iota(jnp.int32, (rank, total * rank), 1)
    mix = jnp.where(col < my * rank, mm(lam_my, c_all, NT),
                    jnp.where(col >= (my + 1) * rank, mm(c_my, lam_all, NT), 0.0))
    v = -mm(c_my, jnp.concatenate(scaled_c, axis=0), NT)
    m1 = (c_my.astype(jnp.float32) * scale).astype(bf)
    m2 = (-c_my.astype(jnp.float32) * beta).astype(bf)
    return m1, m2, lam_my, mix, v


def kernel(sizes, len_hbm, keep_hbm, gain_hbm, e_hbm, g_hbm, d_hbm, u_hbm, out_ref, gout_ref,
           len_ref, keep_ref, gain_ref, e_ref, g_ref, d_ref, u_ref, every, own_all, gram_tx, gram_rx, gram_all,
           tx, xrx, ztx, zrx, hold, gtx, grx, garx, mix_tx, mix_xrx, mix_ztx, mix_zrx, mix_all, arx,
           load_sem, s1, r1, f1, s2, r2, s3, r3, s4, r4, sx, rx, sz, rz, sg, rg, sga, rga,
           smx, rmx, smz, rmz, smb, rmb, saz, raz, sax, rax):
    total, groups, inner, rank, micro, tok, width, part, model = sizes
    rows = micro * tok
    outer = groups // inner
    chunks = width // part
    halves = 2 if part % 256 == 0 and part > 256 else 1
    sub = part // halves
    tiles = sub // 128
    bf, f32 = jnp.bfloat16, jnp.float32
    my = lax.axis_index("section")
    me = lax.axis_index("dp")
    z = me // inner
    x = me % inner

    def lanes(c):
        return pl.ds(pl.multiple_of(c * part, part), part)

    def ranks(s):
        return pl.ds(pl.multiple_of(s * rank, rank), rank)

    mine = jnp.minimum(me, chunks - 1)
    loads = [pltpu.make_async_copy(a, b, load_sem.at[i]) for i, (a, b) in enumerate(
        [(u_hbm.at[:, lanes(mine)], every.at[1, ranks(my), :]),
         (gain_hbm, gain_ref), (keep_hbm, keep_ref), (len_hbm, len_ref),
         (e_hbm, e_ref), (d_hbm, d_ref), (u_hbm, u_ref), (g_hbm, g_ref)])]
    for load in loads:
        load.start()

    barrier = pltpu.get_barrier_semaphore()

    def greet_section(k, c):
        pl.semaphore_signal(barrier, inc=1, device_id={"section": (my + k) % total}, device_id_type=MESH)
        return c

    def greet_dp(k, c):
        pl.semaphore_signal(barrier, inc=1, device_id={"dp": (me + k) % groups}, device_id_type=MESH)
        return c

    lax.fori_loop(1, total, greet_section, 0)
    lax.fori_loop(1, groups, greet_dp, 0)

    def remote(src, dst, send, recv, **where):
        return pltpu.make_async_remote_copy(src_ref=src, dst_ref=dst, send_sem=send, recv_sem=recv,
                                            device_id=where, device_id_type=MESH)

    for i in range(4):
        loads[i].wait()
    real = jnp.where(me < chunks, 1.0, 0.0).astype(f32)
    if chunks < groups:
        every[1, ranks(my), :] = (every[1, ranks(my), :].astype(f32) * real).astype(bf)

    lane = lax.broadcasted_iota(jnp.int32, (1, rows), 1)
    valid = jnp.zeros((1, rows), f32)
    for m in range(micro):
        valid = valid + jnp.where((lane >= m * tok) & (lane < m * tok + len_ref[0, m]), 1.0, 0.0)
    row8 = lax.broadcasted_iota(jnp.int32, (micro, rows), 0) * tok
    lane8 = lax.broadcasted_iota(jnp.int32, (micro, rows), 1)
    member = jnp.where((lane8 >= row8) & (lane8 < row8 + tok), 1.0, 0.0).astype(f32)
    row16 = lax.broadcasted_iota(jnp.int32, (tok, rows), 0)
    lane16 = lax.broadcasted_iota(jnp.int32, (tok, rows), 1)
    spread = jnp.zeros((tok, rows), f32)
    for m in range(micro):
        spread = spread + jnp.where(lane16 == row16 + m * tok, 1.0, 0.0)
    kept_row = valid * jnp.sum(mm(keep_ref[...].astype(f32), spread) * member, axis=0, keepdims=True)

    pl.semaphore_wait(barrier, total + groups - 2)

    step = 2 if total % 2 == 0 else 1
    mate = my + 1 - 2 * (my % 2)

    def block(w, src):
        return every.at[w, ranks(src), :]

    def weights(w, j, src):
        return remote(block(w, src), block(w, src), s1.at[w, j], r1.at[w, src], section=j)

    def share(w, src):
        return remote(block(w, src), block(w, src), f1.at[w, src], r1.at[w, src], section=mate)

    def send_weights(w):
        for k in range(step, total, step):
            weights(w, (my + k) % total, my).start()
        if step == 2:
            weights(w, mate, my).start()

    def pass_weights(w):
        for k in range(step, total, step):
            src = (my + k) % total
            weights(w, my, src).wait_recv()
            if step == 2:
                share(w, src).start()

    def wait_weights(w):
        if step == 2:
            for k in range(0, total, 2):
                weights(w, my, (mate + k) % total).wait_recv()

    send_weights(1)
    for i in range(4, 7):
        loads[i].wait()

    def entry_chunk(c, acc):
        e = e_ref[:, lanes(c)]
        a = (d_ref[:, lanes(c)].astype(f32) * gain_ref[:, lanes(c)].astype(f32)).astype(bf)
        return (acc[0] + mm(jnp.concatenate([a, u_ref[:, lanes(c)]], axis=0), e, NT),
                acc[1] + mm(jnp.ones((8, part), bf), e * e, NT))

    zero = jnp.zeros((rank, rows), f32)
    sums = (jnp.zeros((2 * rank, rows), f32), jnp.zeros((8, rows), f32))
    aue, nn = lax.fori_loop(0, chunks, entry_chunk, sums)
    loads[7].wait()
    ug = lax.fori_loop(0, chunks, lambda c, acc: acc + mm(u_ref[:, lanes(c)], g_ref[:, lanes(c)], NT), zero)
    own_all[my] = jnp.concatenate([aue, ug, nn, jnp.broadcast_to(kept_row, (8, rows))], axis=0)

    def owns(j, src):
        return remote(own_all.at[src], own_all.at[src], s2.at[j], r2.at[src], section=j)

    for k in range(1, total):
        owns((my + k) % total, my).start()
    every[0, ranks(my), :] = (d_ref[:, lanes(mine)].astype(f32) * gain_ref[:, lanes(mine)].astype(f32)
                              * real).astype(bf)
    send_weights(0)

    pass_weights(1)
    wait_weights(1)
    size = total * rank
    col = lax.broadcasted_iota(jnp.int32, (rank, size), 1)
    both = mm(jnp.concatenate([every[0, ranks(my), :], every[1, ranks(my), :]], axis=0), every[1], NT)
    gram_tx[...] = jnp.where(col < my * rank, both[:rank], both[rank:]).astype(bf)

    def grams(j, src):
        return remote(gram_tx, gram_rx.at[src], s3.at[j], r3.at[src], dp=j)

    def send_gram(k, c):
        grams((me + k) % groups, me).start()
        return c

    lax.fori_loop(1, groups, send_gram, 0)
    pass_weights(0)
    gram_rx[me] = gram_tx[...]

    def wait_gram(k, c):
        grams(me, (me + k) % groups).wait_recv()
        return c

    lax.fori_loop(1, groups, wait_gram, 0)
    gram = lax.fori_loop(0, groups, lambda k, acc: acc + gram_rx[k].astype(f32), jnp.zeros((rank, size), f32))
    gram_all[ranks(my), :] = gram.astype(bf)

    def all_grams(j, src):
        return remote(gram_all.at[ranks(src), :], gram_all.at[ranks(src), :], s4.at[j], r4.at[src], section=j)

    for k in range(1, total):
        all_grams((my + k) % total, my).start()
    for k in range(1, total):
        owns(my, (my + k) % total).wait_recv()
    for k in range(1, total):
        all_grams(my, (my + k) % total).wait_recv()

    table = gram_all[...]
    eye = jnp.where(lax.broadcasted_iota(jnp.int32, (size, size), 0)
                    == lax.broadcasted_iota(jnp.int32, (size, size), 1), 1.0, 0.0).astype(bf)
    turned = mm(table, eye, TN)
    au = [table[s * rank:(s + 1) * rank] for s in range(total)]
    uu = [jnp.where(col >= s * rank, au[s].astype(f32), turned[s * rank:(s + 1) * rank]).astype(bf)
          for s in range(total)]
    own = [own_all[s] for s in range(total)]
    kept = [own_all[s, 3 * rank + 8:3 * rank + 9] for s in range(total)]
    m1, m2, lam, mix, v = solve(au, uu, own, kept, valid, member, model, my)

    left = jnp.concatenate([jnp.concatenate([m1, m2], axis=1),
                            jnp.concatenate([jnp.zeros_like(lam), lam], axis=1)], axis=0)

    peer = me + 1 - 2 * x
    near_end = jnp.minimum(z, outer - 1 - z)
    lead = outer - 1 - 2 * near_end

    def far(k):
        j = jnp.maximum(k - lead, 0)
        inner_q = jnp.where(j % 2 == 0, 2 * near_end - j // 2, j // 2)
        q = jnp.where(k < lead, outer - 1 - k, inner_q)
        return jnp.where(z > near_end, outer - 1 - q, q)

    def columns(c, h):
        return pl.ds(pl.multiple_of(c * part + h * sub, sub), sub)

    def piece(c, h):
        at = columns(c, h)
        both = mm(left, jnp.concatenate([g_ref[:, at], e_ref[:, at]], axis=0))
        row = jnp.sum(d_ref[:, at].astype(f32) * both[rank:], axis=0, keepdims=True)
        return both[:rank], row

    def put_row(c, h, row):
        for i in range(tiles):
            gtx[c, h * tiles + i:h * tiles + i + 1, :] = row[:, 128 * i:128 * (i + 1)]

    def mix_x():
        return remote(mix_tx.at[1 - x], mix_xrx, smx, rmx, dp=peer)

    def mix_z(q, src):
        return remote(mix_ztx, mix_zrx.at[src], smz.at[q], rmz.at[src], dp=q * inner + x)

    def mix_back(side):
        return remote(mix_all.at[side], mix_all.at[side], smb, rmb, dp=peer)

    def send_x(p):
        return remote(tx.at[p], xrx.at[p], sx.at[p], rx.at[p], dp=peer)

    def send_z(way, p):
        return remote(ztx.at[p], zrx.at[way, p], sz.at[p], rz.at[way, p], dp=(z + 1 - 2 * way) * inner + x)

    def send_row(c, src):
        return remote(gtx.at[c], grx.at[src], sg.at[c], rg.at[src], dp=c)

    def give_z(way, p):
        return remote(arx.at[p], arx.at[p], saz.at[way, p], raz.at[p], dp=(z + 1 - 2 * way) * inner + x)

    def give_x(p):
        return remote(arx.at[p], arx.at[p], sax.at[p], rax.at[p], dp=peer)

    def give_row(j, src):
        return remote(garx.at[src], garx.at[src], sga.at[j], rga.at[src], dp=j)

    mix_tx[0] = mix.astype(bf)
    mix_tx[1] = v.astype(bf)
    mix_x().start()

    def first(k, carry):
        q = far(k)
        c = q * inner + 1 - x
        for h in range(halves):
            big, row = piece(jnp.minimum(c, chunks - 1), h)
            tx[q * halves + h] = big.astype(bf)
            put_row(c, h, row)
            send_x(q * halves + h).start()
        send_row(c, me).start()
        return carry

    lax.fori_loop(0, outer, first, 0)
    mix_x().wait_recv()
    mix_ztx[...] = (mix_tx[x].astype(f32) + mix_xrx[...].astype(f32)).astype(bf)
    for k in range(1, outer):
        mix_z((z + k) % outer, z).start()

    def second(k, carry):
        q = far(k)
        c = q * inner + x
        way = jnp.where(q > z, 0, 1)
        behind = jnp.where(q > z, z, outer - 1 - z)
        for h in range(halves):
            p = q * halves + h
            big, row = piece(jnp.minimum(c, chunks - 1), h)
            put_row(c, h, row)
            send_x(p).wait_recv()
            hold[...] = big + xrx[p].astype(f32)

            @pl.when(behind > 0)
            def _():
                send_z(way, p).wait_recv()
                hold[...] = hold[...] + zrx[way, p].astype(f32)

            ztx[p] = hold[...].astype(bf)
            send_z(way, p).start()
        send_row(c, me).start()
        return carry

    lax.fori_loop(0, outer - 1, second, 0)

    mixed = mix_ztx[...].astype(f32)
    for k in range(1, outer):
        q = (z + k) % outer
        mix_z(z, q).wait_recv()
        mixed = mixed + mix_zrx[q].astype(f32)
    mix_all[x] = mixed.astype(bf)
    mix_back(x).start()
    wait_weights(0)
    mine_parts = [piece(mine, h) for h in range(halves)]
    mix_back(1 - x).wait_recv()
    low = jnp.where(col < my * rank, mix_all[0].astype(f32), 0.0).astype(bf)
    high = jnp.where(col < my * rank, 0.0, mix_all[0].astype(f32)).astype(bf)
    for h in range(halves):
        big, row = mine_parts[h]
        p = z * halves + h
        at = slice(h * sub, (h + 1) * sub)
        big = big + mm(high, every[0, :, at]) + mm(mix_all[1], every[1, :, at])
        row = row + jnp.sum(d_ref[:, columns(mine, h)].astype(f32) * mm(low, every[1, :, at]), axis=0, keepdims=True)
        put_row(me, h, row)
        send_x(p).wait_recv()
        hold[...] = big + xrx[p].astype(f32)
        for way, behind in ((0, z), (1, outer - 1 - z)):
            @pl.when(behind > 0)
            def _():
                send_z(way, p).wait_recv()
                hold[...] = hold[...] + zrx[way, p].astype(f32)

        p = me * halves + h
        arx[p] = hold[...].astype(bf)
        for way, behind in ((0, outer - 1 - z), (1, z)):
            @pl.when(behind > 0)
            def _():
                give_z(way, p).start()

        give_x(p).start()

    def add_row(k, acc):
        src = (me + k) % groups
        send_row(me, src).wait_recv()
        return acc + grx[src]

    garx[me] = lax.fori_loop(1, groups, add_row, gtx[me])

    def spread_row(k, carry):
        give_row((me + k) % groups, me).start()
        return carry

    lax.fori_loop(1, groups, spread_row, 0)

    def write(c, h):
        def go():
            out_ref[:, columns(c, h)] = arx[c * halves + h]
        if chunks == groups:
            go()
        else:
            pl.when(c < chunks)(go)

    def pass_on(k, carry):
        q = far(outer - 2 - k)
        c = q * inner + x
        way = jnp.where(q < z, 0, 1)
        ahead = jnp.where(q < z, outer - 1 - z, z)
        for h in range(halves):
            p = c * halves + h
            give_z(way, p).wait_recv()

            @pl.when(ahead > 0)
            def _():
                give_z(way, p).start()

            give_x(p).start()
            write(c, h)
        return carry

    lax.fori_loop(0, outer - 1, pass_on, 0)
    for h in range(halves):
        write(me, h)

    def write_row(c, carry):
        for i in range(part // 128):
            gout_ref[:, pl.ds(pl.multiple_of(c * part + 128 * i, 128), 128)] = garx[c, i:i + 1, :]
        return carry

    def wait_row(k, carry):
        give_row(me, (me + k) % groups).wait_recv()
        return carry

    lax.fori_loop(1, groups, wait_row, 0)
    lax.fori_loop(0, chunks, write_row, 0)

    def last(k, carry):
        c = far(outer - 1 - k) * inner + 1 - x
        for h in range(halves):
            give_x(c * halves + h).wait_recv()
            write(c, h)
        return carry

    lax.fori_loop(0, outer, last, 0)

    for w in range(2):
        for k in range(step, total, step):
            weights(w, (my + k) % total, my).wait_send()
            if step == 2:
                share(w, (my + k) % total).wait_send()
        if step == 2:
            weights(w, mate, my).wait_send()
    for k in range(1, total):
        j = (my + k) % total
        owns(j, my).wait_send()
        all_grams(j, my).wait_send()
    mix_x().wait_send()
    mix_back(x).wait_send()
    for h in range(halves):
        p = me * halves + h
        for way, behind in ((0, outer - 1 - z), (1, z)):
            @pl.when(behind > 0)
            def _():
                give_z(way, p).wait_send()

    def left_dp(k, carry):
        j = (me + k) % groups
        grams(j, me).wait_send()
        send_row(j, me).wait_send()
        give_row(j, me).wait_send()
        return carry

    lax.fori_loop(1, groups, left_dp, 0)

    def left_z(k, carry):
        q = (z + k) % outer
        mix_z(q, z).wait_send()
        ahead = jnp.where(q < z, outer - 1 - z, z)
        for h in range(halves):
            send_z(jnp.where(q > z, 0, 1), q * halves + h).wait_send()

            @pl.when(ahead > 0)
            def _():
                give_z(jnp.where(q < z, 0, 1), (q * inner + x) * halves + h).wait_send()
        return carry

    lax.fori_loop(1, outer, left_z, 0)

    def left_x(q, carry):
        for h in range(halves):
            send_x(q * halves + h).wait_send()
            give_x((q * inner + x) * halves + h).wait_send()
        return carry

    lax.fori_loop(0, outer, left_x, 0)


def body(entry, gain, down, up, gout, lengths, keep):
    bf, f32 = jnp.bfloat16, jnp.float32
    total = lax.axis_size("section")
    groups = lax.axis_size("dp")
    micro, tok, width = entry.shape[1:]
    rank = down.shape[1]
    rows = micro * tok
    part = 128 * (-(-width // (128 * groups)))
    pad = -width % part
    wide = width + pad
    inner = 2
    halves = 2 if part % 256 == 0 and part > 256 else 1
    sub = part // halves
    outer = groups // inner
    widen = lambda a: jnp.pad(a, ((0, 0), (0, pad))) if pad else a
    hold = lambda a: pltpu.with_memory_space_constraint(a, pltpu.HBM)
    e = hold(widen(entry[0].reshape(rows, width)))
    go = hold(widen(gout[0].reshape(rows, width)))
    d, u = hold(widen(down[0])), hold(widen(up[0]))
    tall = max(8, part // 128)
    pieces = outer * halves
    sizes = (total, groups, inner, rank, micro, tok, wide, part, width)
    vm = lambda *s, t=bf: pltpu.VMEM(s, t)
    dma = lambda *n: pltpu.SemaphoreType.DMA(n)
    one = pltpu.SemaphoreType.DMA
    scratch = [
        pltpu.SMEM((1, micro), jnp.int32), vm(micro, tok, t=jnp.int32), vm(1, wide),
        vm(rows, wide), vm(rows, wide), vm(rank, wide), vm(rank, wide),
        vm(2, total * rank, part),
        vm(total, 3 * rank + 16, rows, t=f32),
        vm(rank, total * rank), vm(groups, rank, total * rank), vm(total * rank, total * rank),
        vm(pieces, rank, sub), vm(pieces, rank, sub), vm(pieces, rank, sub), vm(2, pieces, rank, sub),
        vm(rank, sub, t=f32),
        vm(groups, tall, 128, t=f32), vm(groups, tall, 128, t=f32), vm(groups, tall, 128, t=f32),
        vm(2, rank, total * rank), vm(rank, total * rank), vm(rank, total * rank),
        vm(outer, rank, total * rank), vm(2, rank, total * rank),
        vm(groups * halves, rank, sub),
        dma(8), dma(2, total), dma(2, total), dma(2, total), dma(total), dma(total), dma(groups), dma(groups),
        dma(total), dma(total),
        dma(pieces), dma(pieces), dma(pieces), dma(2, pieces), dma(groups), dma(groups), dma(groups), dma(groups),
        one, one, dma(outer), dma(outer), one, one,
        dma(2, groups * halves), dma(groups * halves), dma(groups * halves), dma(groups * halves),
    ]
    inside = pl.BlockSpec(memory_space=pltpu.VMEM)
    outside = pl.BlockSpec(memory_space=pltpu.HBM)
    up_grad, gain_grad = pl.pallas_call(
        functools.partial(kernel, sizes),
        out_shape=(jax.ShapeDtypeStruct((rank, wide), bf), jax.ShapeDtypeStruct((1, wide), f32)),
        in_specs=[outside] * 7,
        out_specs=(inside, inside),
        scratch_shapes=scratch,
        compiler_params=pltpu.CompilerParams(
            collective_id=0, has_side_effects=True, vmem_limit_bytes=48 * 1024 * 1024),
        name="relay",
    )(hold(lengths), hold(keep[0, 0]), hold(widen(gain)), e, go, d, u)
    return up_grad[None, :, :width].astype(f32), gain_grad[:, :width]


def solution(mesh):
    in_specs = (
        P("dp", None, None, None),
        P("section", None),
        P("section", None, None),
        P("section", None, None),
        P("dp", None, None, None),
        P("dp", None),
        P("dp", "section", None, None),
    )
    out_specs = (P("section", None, None), P("section", None))
    return jax.shard_map(body, mesh=mesh, in_specs=in_specs, out_specs=out_specs, check_vma=False)
```

```python
import functools

import jax
import jax.numpy as jnp
from jax import lax
from jax.experimental import pallas as pl
from jax.experimental.pallas import tpu as pltpu
from jax.sharding import PartitionSpec as P

EPS = 1e-05
NT = (((1,), (1,)), ((), ()))
TN = (((0,), (0,)), ((), ()))
MESH = pl.DeviceIdType.MESH
NN = (((1,), (0,)), ((), ()))


def mm(a, b, dims=NN, precision=None):
    return lax.dot_general(a, b, dims, precision=precision, preferred_element_type=jnp.float32)


def solve(au, uu, own, kept, valid, member, width, my):
    total, (rank, _) = len(au), au[0].shape
    rows = own[0].shape[1]
    bf = jnp.bfloat16
    norm2 = own[0][3 * rank:3 * rank + 1]
    r_now = jnp.concatenate([own[s][rank:2 * rank] for s in range(total)], axis=0)
    acc = jnp.concatenate([own[s][2 * rank:3 * rank] for s in range(total)], axis=0)
    zero = jnp.zeros((rank, rows), bf)
    cs, ps, invs, rs = [], [], [], []
    energy = jnp.zeros((1, rows), jnp.float32)
    count = jnp.zeros((1, rows), jnp.float32)
    for s in range(total):
        inv = lax.rsqrt(norm2 * (1.0 / width) + EPS)
        p = own[s][:rank]
        if s:
            p = p + mm(au[s], jnp.concatenate(cs + [zero] * (total - s), axis=0))
        c = (kept[s] * (p * inv).astype(bf).astype(jnp.float32)).astype(bf)
        cf = c.astype(jnp.float32)
        g = mm(uu[s], c, TN)
        quad = jnp.sum(cf * g[s * rank:(s + 1) * rank], axis=0, keepdims=True)
        cross = jnp.sum(cf * r_now[s * rank:(s + 1) * rank], axis=0, keepdims=True)
        rs.append(r_now)
        energy = energy + quad
        count = count + kept[s]
        norm2 = norm2 + 2.0 * cross + quad
        r_now = r_now + g
        cs.append(c)
        ps.append(p)
        invs.append(inv)
    sums = jnp.concatenate([energy, count, jnp.zeros((6, rows), jnp.float32)], axis=0)
    sums = mm(mm(sums, member, NT, lax.Precision.HIGHEST), member, NN, lax.Precision.HIGHEST)
    energy, count = sums[0:1], sums[1:2]
    scale = valid / (count * jnp.sqrt(energy / (width * count) + EPS))
    acc = acc * scale
    lams, alphas = [None] * total, [None] * total
    for s in reversed(range(total)):
        lam = (kept[s] * acc[s * rank:(s + 1) * rank]).astype(bf)
        lf = lam.astype(jnp.float32)
        alpha = invs[s] * invs[s] * invs[s] * jnp.sum(lf * ps[s], axis=0, keepdims=True) * (1.0 / width)
        lams[s] = (lf * invs[s]).astype(bf)
        alphas[s] = alpha
        if s:
            acc = acc + invs[s] * mm(au[s], lam, TN) - alpha * rs[s]
    c_all = jnp.concatenate(cs, axis=0)
    lam_all = jnp.concatenate(lams, axis=0)
    fl = lambda cond: jnp.where(cond, 1.0, 0.0).astype(jnp.float32)
    c_my = sum(fl(my == s) * cs[s].astype(jnp.float32) for s in range(total)).astype(bf)
    lam_my = sum(fl(my == s) * lams[s].astype(jnp.float32) for s in range(total)).astype(bf)
    beta = sum(fl(j > my) * alphas[j] for j in range(total))
    scaled_c = []
    for i in range(total):
        b = jnp.zeros((1, rows), jnp.float32)
        for j in range(i + 1, total):
            b = b + fl(j > my) * alphas[j]
        scaled_c.append((cs[i].astype(jnp.float32) * b).astype(bf))
    col = lax.broadcasted_iota(jnp.int32, (rank, total * rank), 1)
    mix = jnp.where(col < my * rank, mm(lam_my, c_all, NT),
                    jnp.where(col >= (my + 1) * rank, mm(c_my, lam_all, NT), 0.0))
    v = -mm(c_my, jnp.concatenate(scaled_c, axis=0), NT)
    m1 = (c_my.astype(jnp.float32) * scale).astype(bf)
    m2 = (-c_my.astype(jnp.float32) * beta).astype(bf)
    return m1, m2, lam_my, mix, v


def kernel(sizes, len_hbm, keep_hbm, gain_hbm, e_hbm, g_hbm, d_hbm, u_hbm, out_ref, gout_ref,
           len_ref, keep_ref, gain_ref, e_ref, g_ref, d_ref, u_ref, every, own_all, gram_tx, gram_rx, gram_all,
           tx, xrx, ztx, zrx, zend, gtx, grx, garx, mix_tx, mix_xrx, mix_ztx, mix_zrx, mix_all, arx,
           load_sem, s1, r1, rm, s2, r2, s3, r3, s4, r4, sx, rx, sz, rz, rze, sg, rg, sga, rga,
           smx, rmx, smz, rmz, smb, rmb, saz, raz, sax, rax):
    total, groups, inner, rank, micro, tok, width, part, model = sizes
    rows = micro * tok
    outer = groups // inner
    chunks = width // part
    halves = 2 if part % 256 == 0 and part > 256 else 1
    sub = part // halves
    tiles = sub // 128
    bf, f32 = jnp.bfloat16, jnp.float32
    my = lax.axis_index("section")
    me = lax.axis_index("dp")
    z = me // inner
    x = me % inner

    def lanes(c):
        return pl.ds(pl.multiple_of(c * part, part), part)

    def ranks(s):
        return pl.ds(pl.multiple_of(s * rank, rank), rank)

    mine = jnp.minimum(me, chunks - 1)
    loads = [pltpu.make_async_copy(a, b, load_sem.at[i]) for i, (a, b) in enumerate(
        [(u_hbm.at[:, lanes(mine)], every.at[1, ranks(my), :]),
         (gain_hbm, gain_ref), (keep_hbm, keep_ref), (len_hbm, len_ref),
         (e_hbm, e_ref), (d_hbm, d_ref), (u_hbm, u_ref), (g_hbm, g_ref)])]
    for load in loads:
        load.start()

    barrier = pltpu.get_barrier_semaphore()

    def greet_section(k, c):
        pl.semaphore_signal(barrier, inc=1, device_id={"section": (my + k) % total}, device_id_type=MESH)
        return c

    def greet_dp(k, c):
        pl.semaphore_signal(barrier, inc=1, device_id={"dp": (me + k) % groups}, device_id_type=MESH)
        return c

    lax.fori_loop(1, total, greet_section, 0)
    lax.fori_loop(1, groups, greet_dp, 0)

    def remote(src, dst, send, recv, **where):
        return pltpu.make_async_remote_copy(src_ref=src, dst_ref=dst, send_sem=send, recv_sem=recv,
                                            device_id=where, device_id_type=MESH)

    real = jnp.where(me < chunks, 1.0, 0.0).astype(f32)
    loads[0].wait()
    if chunks < groups:
        every[1, ranks(my), :] = (every[1, ranks(my), :].astype(f32) * real).astype(bf)
    pl.semaphore_wait(barrier, total + groups - 2)

    step = 2 if total % 2 == 0 else 1
    mate = my + 1 - 2 * (my % 2)

    def block(w, src):
        return every.at[w, ranks(src), :]

    def weights(w, j, src):
        return remote(block(w, src), block(w, src), s1, r1.at[w, src // step], section=j)

    def share(w, src):
        return remote(block(w, src), block(w, src), s1, rm.at[w], section=mate)

    def send_weights(w):
        for k in range(step, total, step):
            weights(w, (my + k) % total, my).start()
        if step == 2:
            share(w, my).start()

    def pass_weights(w):
        for k in range(step, total, step):
            src = (my + k) % total
            weights(w, my, src).wait_recv()
            if step == 2:
                share(w, src).start()

    def wait_weights(w):
        if step == 2:
            part_of = every.at[w, pl.ds(0, total // 2 * rank), :]
            remote(part_of, part_of, s1, rm.at[w], section=mate).wait_recv()

    send_weights(1)
    for i in range(1, 4):
        loads[i].wait()
    lane = lax.broadcasted_iota(jnp.int32, (1, rows), 1)
    valid = jnp.zeros((1, rows), f32)
    for m in range(micro):
        valid = valid + jnp.where((lane >= m * tok) & (lane < m * tok + len_ref[0, m]), 1.0, 0.0)
    row8 = lax.broadcasted_iota(jnp.int32, (micro, rows), 0) * tok
    lane8 = lax.broadcasted_iota(jnp.int32, (micro, rows), 1)
    member = jnp.where((lane8 >= row8) & (lane8 < row8 + tok), 1.0, 0.0).astype(f32)
    row16 = lax.broadcasted_iota(jnp.int32, (tok, rows), 0)
    lane16 = lax.broadcasted_iota(jnp.int32, (tok, rows), 1)
    spread = jnp.zeros((tok, rows), f32)
    for m in range(micro):
        spread = spread + jnp.where(lane16 == row16 + m * tok, 1.0, 0.0)
    kept_row = valid * jnp.sum(mm(keep_ref[...].astype(f32), spread) * member, axis=0, keepdims=True)

    for i in range(4, 7):
        loads[i].wait()

    def entry_chunk(c, acc):
        e = e_ref[:, lanes(c)]
        a = (d_ref[:, lanes(c)].astype(f32) * gain_ref[:, lanes(c)].astype(f32)).astype(bf)
        return (acc[0] + mm(jnp.concatenate([a, u_ref[:, lanes(c)]], axis=0), e, NT),
                acc[1] + mm(jnp.ones((8, part), bf), e * e, NT))

    zero = jnp.zeros((rank, rows), f32)
    sums = (jnp.zeros((2 * rank, rows), f32), jnp.zeros((8, rows), f32))
    aue, nn = lax.fori_loop(0, chunks, entry_chunk, sums)
    every[0, ranks(my), :] = (d_ref[:, lanes(mine)].astype(f32) * gain_ref[:, lanes(mine)].astype(f32)
                              * real).astype(bf)
    pass_weights(1)
    loads[7].wait()

    def out_chunk(c, acc):
        return acc + mm(u_ref[:, lanes(c)], g_ref[:, lanes(c)], NT)

    ug = lax.fori_loop(0, chunks // 2, out_chunk, zero)
    wait_weights(1)
    size = total * rank
    col = lax.broadcasted_iota(jnp.int32, (rank, size), 1)
    both = mm(jnp.concatenate([every[0, ranks(my), :], every[1, ranks(my), :]], axis=0), every[1], NT)
    gram_tx[...] = jnp.where(col < my * rank, both[:rank], both[rank:]).astype(bf)

    def grams(j, src):
        return remote(gram_tx, gram_rx.at[src], s3, r3, dp=j)

    def send_gram(k, c):
        grams((me + k) % groups, me).start()
        return c

    lax.fori_loop(1, groups, send_gram, 0)
    gram_rx[me] = gram_tx[...]
    ug = lax.fori_loop(chunks // 2, chunks, out_chunk, ug)
    own_all[my] = jnp.concatenate([aue, ug, nn, jnp.broadcast_to(kept_row, (8, rows))], axis=0)

    def owns(j, src):
        return remote(own_all.at[src], own_all.at[src], s2, r2, section=j)

    for k in range(1, total):
        owns((my + k) % total, my).start()
    others = gram_rx.at[pl.ds(0, groups - 1)]
    all_of_grams = remote(others, others, s3, r3, dp=me)
    all_of_grams.wait_recv()
    gram = lax.fori_loop(0, groups, lambda k, acc: acc + gram_rx[k].astype(f32), jnp.zeros((rank, size), f32))
    gram_all[ranks(my), :] = gram.astype(bf)

    def all_grams(j, src):
        return remote(gram_all.at[ranks(src), :], gram_all.at[ranks(src), :], s4, r4, section=j)

    for k in range(1, total):
        all_grams((my + k) % total, my).start()
    send_weights(0)
    others = own_all.at[pl.ds(0, total - 1)]
    all_of_owns = remote(others, others, s2, r2, section=my)
    all_of_owns.wait_recv()
    others = gram_all.at[pl.ds(0, (total - 1) * rank), :]
    all_of_tables = remote(others, others, s4, r4, section=my)
    all_of_tables.wait_recv()

    table = gram_all[...]
    eye = jnp.where(lax.broadcasted_iota(jnp.int32, (size, size), 0)
                    == lax.broadcasted_iota(jnp.int32, (size, size), 1), 1.0, 0.0).astype(bf)
    turned = mm(table, eye, TN)
    au = [table[s * rank:(s + 1) * rank] for s in range(total)]
    uu = [jnp.where(col >= s * rank, au[s].astype(f32), turned[s * rank:(s + 1) * rank]).astype(bf)
          for s in range(total)]
    own = [own_all[s] for s in range(total)]
    kept = [own_all[s, 3 * rank + 8:3 * rank + 9] for s in range(total)]
    m1, m2, lam, mix, v = solve(au, uu, own, kept, valid, member, model, my)

    left = jnp.concatenate([jnp.concatenate([m1, m2], axis=1),
                            jnp.concatenate([jnp.zeros_like(lam), lam], axis=1)], axis=0)

    peer = me + 1 - 2 * x
    twin = z + 1 - 2 * (z % 2)
    pairs = outer // 2

    def across(k, side):
        return 2 * ((z // 2 + 1 + k) % pairs) + side

    def order(k):
        own_side = jnp.where(k < outer - 2, across(k - pairs + 1, z % 2), jnp.where(k < outer - 1, twin, z))
        return jnp.where(k < pairs - 1, across(k, twin % 2), own_side)

    def columns(c, h):
        return pl.ds(pl.multiple_of(c * part + h * sub, sub), sub)

    def piece(c, h):
        at = columns(c, h)
        both = mm(left, jnp.concatenate([g_ref[:, at], e_ref[:, at]], axis=0))
        row = jnp.sum(d_ref[:, at].astype(f32) * both[rank:], axis=0, keepdims=True)
        return both[:rank], row

    def put_row(c, h, row):
        for i in range(tiles):
            gtx[c, h * tiles + i:h * tiles + i + 1, :] = row[:, 128 * i:128 * (i + 1)]

    def mix_x():
        return remote(mix_tx.at[1 - x], mix_xrx, smx, rmx, dp=peer)

    def mix_z(q, src):
        return remote(mix_ztx, mix_zrx.at[src], smz, rmz, dp=q * inner + x)

    def mix_back(side):
        return remote(mix_all.at[side], mix_all.at[side], smb, rmb, dp=peer)

    def send_x(p):
        return remote(tx.at[p], xrx.at[p], sx, rx.at[p], dp=peer)

    def send_end(q, h, src):
        return remote(ztx.at[q * halves + h], zend.at[src * halves + h], sz, rze.at[src * halves + h], dp=q * inner + x)

    def send_twin(p):
        return remote(ztx.at[p], zrx.at[p], sz, rz.at[p], dp=twin * inner + x)

    def send_row(c):
        return remote(gtx.at[c], grx.at[me], sg, rg, dp=c)

    def give_z(q, src, h):
        p = (src * inner + x) * halves + h
        return remote(arx.at[p], arx.at[p], saz, raz.at[src * halves + h], dp=q * inner + x)

    def give_x(q, side, h):
        p = (q * inner + side) * halves + h
        return remote(arx.at[p], arx.at[p], sax, rax.at[q * halves + h], dp=peer)

    def give_row(j):
        return remote(garx.at[me], garx.at[me], sga, rga, dp=j)

    def batch(ref, count, send, recv):
        some = ref.at[pl.ds(0, count)]
        return remote(some, some, send, recv, dp=peer)

    mix_tx[0] = mix.astype(bf)
    mix_tx[1] = v.astype(bf)
    mix_x().start()

    def first(k, carry):
        q = order(k)
        c = q * inner + 1 - x
        for h in range(halves):
            big, row = piece(jnp.minimum(c, chunks - 1), h)
            tx[q * halves + h] = big.astype(bf)
            put_row(c, h, row)
            send_x(q * halves + h).start()
        send_row(c).start()
        return carry

    lax.fori_loop(0, outer, first, 0)
    pass_weights(0)
    mix_x().wait_recv()
    mix_ztx[...] = (mix_tx[x].astype(f32) + mix_xrx[...].astype(f32)).astype(bf)
    for k in range(1, outer):
        mix_z((z + k) % outer, z).start()

    def gather_part(q, h):
        c = q * inner + x
        big, row = piece(jnp.minimum(c, chunks - 1), h)
        put_row(c, h, row)
        send_x(q * halves + h).wait_recv()
        return big + xrx[q * halves + h].astype(f32)

    def to_twin(k, carry):
        q = across(k, twin % 2)
        for h in range(halves):
            ztx[q * halves + h] = gather_part(q, h).astype(bf)
            send_twin(q * halves + h).start()
        send_row(q * inner + x).start()
        return carry

    def to_end(k, carry):
        q = across(k, z % 2)
        for h in range(halves):
            p = q * halves + h
            big = gather_part(q, h)
            send_twin(p).wait_recv()
            ztx[p] = (big + zrx[p].astype(f32)).astype(bf)
            send_end(q, h, z).start()
        send_row(q * inner + x).start()
        return carry

    lax.fori_loop(0, pairs - 1, to_twin, 0)
    lax.fori_loop(0, pairs - 1, to_end, 0)

    mixed = mix_ztx[...].astype(f32)
    batch(mix_zrx, outer - 1, smz, rmz).wait_recv()
    mixed = lax.fori_loop(1, outer, lambda k, acc: acc + mix_zrx[(z + k) % outer].astype(f32), mixed)
    mix_all[x] = mixed.astype(bf)
    mix_back(x).start()

    for h in range(halves):
        ztx[twin * halves + h] = gather_part(twin, h).astype(bf)
        send_end(twin, h, z).start()
    send_row(twin * inner + x).start()
    wait_weights(0)
    mine_parts = [piece(mine, h) for h in range(halves)]
    mix_back(1 - x).wait_recv()
    low = jnp.where(col < my * rank, mix_all[0].astype(f32), 0.0).astype(bf)
    high = jnp.where(col < my * rank, 0.0, mix_all[0].astype(f32)).astype(bf)
    for h in range(halves):
        big, row = mine_parts[h]
        p = z * halves + h
        at = slice(h * sub, (h + 1) * sub)
        big = big + mm(high, every[0, :, at]) + mm(mix_all[1], every[1, :, at])
        row = row + jnp.sum(d_ref[:, columns(mine, h)].astype(f32) * mm(low, every[1, :, at]), axis=0, keepdims=True)
        put_row(me, h, row)
        send_x(p).wait_recv()
        big = big + xrx[p].astype(f32)

        def add_end(k, acc):
            src = across(k, z % 2)
            send_end(z, h, src).wait_recv()
            return acc + zend[src * halves + h].astype(f32)

        big = lax.fori_loop(0, pairs - 1, add_end, big)
        send_end(z, h, twin).wait_recv()
        arx[me * halves + h] = (big + zend[twin * halves + h].astype(f32)).astype(bf)

        def give(k, carry):
            give_z(across(k, z % 2), z, h).start()
            return carry

        lax.fori_loop(0, pairs - 1, give, 0)
        give_z(twin, z, h).start()
        give_x(z, x, h).start()

    batch(grx, groups - 1, sg, rg).wait_recv()
    garx[me] = lax.fori_loop(1, groups, lambda k, acc: acc + grx[(me + k) % groups], gtx[me])

    def spread_row(k, carry):
        give_row((me + k) % groups).start()
        return carry

    lax.fori_loop(1, groups, spread_row, 0)

    def write(c, h):
        def go():
            out_ref[:, columns(c, h)] = arx[c * halves + h]
        if chunks == groups:
            go()
        else:
            pl.when(c < chunks)(go)

    def hand_over(q, h):
        give_x(q, x, h).start()
        write(q * inner + x, h)

    for h in range(halves):
        def from_across(k, carry):
            q = across(k, z % 2)
            give_z(z, q, h).wait_recv()
            give_z(twin, q, h).start()
            hand_over(q, h)
            return carry

        lax.fori_loop(0, pairs - 1, from_across, 0)
        give_z(z, twin, h).wait_recv()
        hand_over(twin, h)

    def from_twin(k, carry):
        q = across(k, twin % 2)
        for h in range(halves):
            give_z(z, q, h).wait_recv()
            hand_over(q, h)
        return carry

    lax.fori_loop(0, pairs - 1, from_twin, 0)
    for h in range(halves):
        write(me, h)

    def write_row(c, carry):
        for i in range(part // 128):
            gout_ref[:, pl.ds(pl.multiple_of(c * part + 128 * i, 128), 128)] = garx[c, i:i + 1, :]
        return carry

    batch(garx, groups - 1, sga, rga).wait_recv()
    lax.fori_loop(0, chunks, write_row, 0)

    def last(q, h):
        give_x(q, 1 - x, h).wait_recv()
        write(q * inner + 1 - x, h)

    for h in range(halves):
        last(z, h)
    for h in range(halves):
        def last_across(k, carry):
            last(across(k, z % 2), h)
            return carry

        lax.fori_loop(0, pairs - 1, last_across, 0)
        last(twin, h)

    def last_twin(k, carry):
        for h in range(halves):
            last(across(k, twin % 2), h)
        return carry

    lax.fori_loop(0, pairs - 1, last_twin, 0)

    sent = every.at[:, pl.ds(0, (total - 1) * rank), :]
    remote(sent, sent, s1, rm.at[0], section=my).wait_send()
    all_of_owns.wait_send()
    all_of_tables.wait_send()
    all_of_grams.wait_send()
    mix_x().wait_send()
    mix_back(x).wait_send()
    batch(mix_zrx, outer - 1, smz, rmz).wait_send()
    batch(gtx, groups - 1, sg, rg).wait_send()
    batch(garx, groups - 1, sga, rga).wait_send()
    batch(tx, outer * halves, sx, rx.at[0]).wait_send()
    batch(ztx, (outer - 1) * halves, sz, rz.at[0]).wait_send()
    batch(arx, outer * halves, sax, rax.at[0]).wait_send()
    batch(arx, (outer - 1) * halves, saz, raz.at[0]).wait_send()


def body(entry, gain, down, up, gout, lengths, keep):
    bf, f32 = jnp.bfloat16, jnp.float32
    total = lax.axis_size("section")
    groups = lax.axis_size("dp")
    micro, tok, width = entry.shape[1:]
    rank = down.shape[1]
    rows = micro * tok
    part = 128 * (-(-width // (128 * groups)))
    pad = -width % part
    wide = width + pad
    inner = 2
    halves = 2 if part % 256 == 0 and part > 256 else 1
    sub = part // halves
    outer = groups // inner
    widen = lambda a: jnp.pad(a, ((0, 0), (0, pad))) if pad else a
    hold = lambda a: pltpu.with_memory_space_constraint(a, pltpu.HBM)
    e = hold(widen(entry[0].reshape(rows, width)))
    go = hold(widen(gout[0].reshape(rows, width)))
    d, u = hold(widen(down[0])), hold(widen(up[0]))
    tall = max(8, part // 128)
    pieces = outer * halves
    sizes = (total, groups, inner, rank, micro, tok, wide, part, width)
    vm = lambda *s, t=bf: pltpu.VMEM(s, t)
    dma = lambda *n: pltpu.SemaphoreType.DMA(n)
    one = pltpu.SemaphoreType.DMA
    scratch = [
        pltpu.SMEM((1, micro), jnp.int32), vm(micro, tok, t=jnp.int32), vm(1, wide),
        vm(rows, wide), vm(rows, wide), vm(rank, wide), vm(rank, wide),
        vm(2, total * rank, part),
        vm(total, 3 * rank + 16, rows, t=f32),
        vm(rank, total * rank), vm(groups, rank, total * rank), vm(total * rank, total * rank),
        *[vm(pieces, rank, sub)] * 5,
        vm(groups, tall, 128, t=f32), vm(groups, tall, 128, t=f32), vm(groups, tall, 128, t=f32),
        vm(2, rank, total * rank), vm(rank, total * rank), vm(rank, total * rank),
        vm(outer, rank, total * rank), vm(2, rank, total * rank),
        vm(groups * halves, rank, sub),
        dma(8), one, dma(2, -(-total // 2) if total % 2 == 0 else total), dma(2), *[one] * 6,
        one, dma(pieces), one, dma(pieces), dma(pieces), *[one] * 4,
        *[one] * 6, one, dma(pieces), one, dma(pieces),
    ]
    inside = pl.BlockSpec(memory_space=pltpu.VMEM)
    outside = pl.BlockSpec(memory_space=pltpu.HBM)
    up_grad, gain_grad = pl.pallas_call(
        functools.partial(kernel, sizes),
        out_shape=(jax.ShapeDtypeStruct((rank, wide), bf), jax.ShapeDtypeStruct((1, wide), f32)),
        in_specs=[outside] * 7,
        out_specs=(inside, inside),
        scratch_shapes=scratch,
        compiler_params=pltpu.CompilerParams(
            collective_id=0, has_side_effects=True, vmem_limit_bytes=48 * 1024 * 1024),
        name="relay",
    )(hold(lengths), hold(keep[0, 0]), hold(widen(gain)), e, go, d, u)
    return up_grad[None, :, :width].astype(f32), gain_grad[:, :width]


def solution(mesh):
    in_specs = (
        P("dp", None, None, None),
        P("section", None),
        P("section", None, None),
        P("section", None, None),
        P("dp", None, None, None),
        P("dp", None),
        P("dp", "section", None, None),
    )
    out_specs = (P("section", None, None), P("section", None))
    return jax.shard_map(body, mesh=mesh, in_specs=in_specs, out_specs=out_specs, check_vma=False)
```
